32 devices in a mesh: dom: 16 (over z, y, x), mem: 2 (over core).
Axes of the slice: x: 2, y: 2, z: 4, core: 2. Of those that a mesh axis runs over, the one named last changes fastest.
Arguments:
- node_latents: bfloat16 [4, 2048, 512], P('mem', 'dom'), may hold values from -6 to 6
- edge_latents: bfloat16 [4, 8192, 512], P('mem', 'dom'), may hold values from -6 to 6
- edge_senders: int32 [8192], P('dom'), may hold values from 0 to 191, as said below
- edge_receivers: int32 [8192], P('dom'), may hold values from 0 to 127
- edge_counts: int32 [16], P('dom'), may hold values from 64 to 512, as said below
- halo_send: int32 [512], P('dom'), may hold values from 0 to 127
- long_send: int32 [16, 16, 2], replicated, may hold values from 0 to 3
- edge_first: bfloat16 [2, 1536, 512], P(None, None, 'mem'), may hold values from -0.15625 to 0.15625
- edge_second: bfloat16 [2, 512, 512], P(None, None, 'mem'), may hold values from -0.25 to 0.25
- node_first: bfloat16 [2, 1024, 512], P(None, None, 'mem'), may hold values from -0.1875 to 0.1875
- node_second: bfloat16 [2, 512, 512], P(None, None, 'mem'), may hold values from -0.25 to 0.25
- edge_gain: float32 [2, 512], replicated, may hold values from 0.5 to 1.5
- edge_shift: float32 [2, 512], replicated, may hold values from -3 to 3
- node_gain: float32 [2, 512], replicated, may hold values from 0.5 to 1.5
- node_shift: float32 [2, 512], replicated, may hold values from -3 to 3
Outputs:
- node_out: bfloat16 [4, 2048, 512], P('mem', 'dom')
- edge_out: bfloat16 [4, 8192, 512], P('mem', 'dom')
The draws below stay inside these ranges and needn't reach their ends.
Inputs may be any that keep to these rules, and one draw needn't show every extreme that they name: `edge_senders`: rows below 128 are the partition's own nodes, the next 32 its neighbours' sent nodes, the rest the coarse slots of all partitions. `edge_counts`: live slots come first in each partition; some partition has exactly 512 live slots.
All inputs are finite; a program needn't handle non-finite values.
Results may differ from the reference program's by a relative error of at most 0.0075.
Values may be sent and summed in bfloat16 or wider, within the bound.
A program may use at most 128 MiB of HBM per device.

```python
import jax
import jax.numpy as jnp
from jax import lax

D = 512
NODE_DEV = 128
EDGE_DEV = 512
HALO = 16
COARSE_DEV = 4
LONG_SLOT = 2
LAYERS = 2
MEMBERS = 4
NODES = 2048
EDGES = 8192
N_DOM = 16


def draw_edge_senders(key, part):
    kind_key = jax.random.fold_in(key, 11)
    local_key = jax.random.fold_in(key, 12)
    halo_key = jax.random.fold_in(key, 13)
    far_key = jax.random.fold_in(key, 14)
    total = N_DOM * EDGE_DEV
    kinds = jax.random.randint(kind_key, (total,), 0, 20)
    local_rows = jax.random.randint(local_key, (total,), 0, NODE_DEV)
    halo_rows = NODE_DEV + jax.random.randint(halo_key, (total,), 0, 2 * HALO)
    far_rows = NODE_DEV + 2 * HALO + jax.random.randint(far_key, (total,), 0, N_DOM * LONG_SLOT)
    picked = jnp.where(kinds < 14, local_rows, jnp.where(kinds < 17, halo_rows, far_rows))
    return picked.astype(jnp.int32)


def draw_edge_counts(key, part):
    count_key = jax.random.fold_in(key, 21)
    place_key = jax.random.fold_in(key, 22)
    counts = jax.random.randint(count_key, (N_DOM,), EDGE_DEV // 8, EDGE_DEV + 1)
    fullest = jax.random.randint(place_key, (), 0, N_DOM)
    counts = jnp.where(jnp.arange(N_DOM) == fullest, EDGE_DEV, counts)
    return counts.astype(jnp.int32)


def set_ends(values, stream_key, smallest, top_value):
    longest = values.shape.index(max(values.shape))
    spots = []
    for shift in (0, 1):
        where = [jax.random.randint(jax.random.fold_in(stream_key, axis), (), 0, length) for axis, length in enumerate(values.shape)]
        where[longest] = (where[longest] + shift) % values.shape[longest]
        spots.append(tuple(where))
    return values.at[spots[0]].set(smallest).at[spots[1]].set(top_value)


def block_levels(stream_key, dims, pieces, least, high):
    def one(dim, blocks):
        heights = jax.random.uniform(jax.random.fold_in(jax.random.fold_in(stream_key, 6), dim), (blocks,), jnp.float32, least / len(pieces), high / len(pieces))
        return jnp.repeat(jnp.exp(heights), dims[dim] // blocks).reshape((-1,) + (1,) * (len(dims) - dim - 1))

    gain = one(*pieces[0])
    for cut in pieces[1:]:
        gain = gain * one(*cut)
    return gain


def noise(stream_key, shape, deviation, most, shards=(), kind=jnp.bfloat16):
    factor_of = block_levels(stream_key, shape, shards, -0.22, 0.18) if shards else 1.0
    drawn = jax.random.normal(stream_key, shape, jnp.float32) * deviation * factor_of
    return jnp.minimum(jnp.maximum(drawn, -most), most).astype(kind)


def setup_inputs(seed: int = 0) -> dict:
    seeds = jax.random.split(jax.random.key(seed), 16)
    node_latents = noise(seeds[0], (MEMBERS, NODES, D), 1.0, 6.0, ((0, 2), (1, 16)))
    edge_latents = noise(seeds[1], (MEMBERS, EDGES, D), 1.0, 6.0, ((0, 2), (1, 16)))
    edge_senders = draw_edge_senders(jax.random.fold_in(seeds[15], 71), 0)
    edge_receivers = set_ends(jax.random.randint(seeds[3], (EDGES,), 0, NODE_DEV), jax.random.fold_in(seeds[3], 1), 0, NODE_DEV - 1).astype(jnp.int32)
    edge_counts = draw_edge_counts(jax.random.fold_in(seeds[15], 71), 0)
    halo_send = set_ends(jax.random.randint(seeds[5], (N_DOM * 2 * HALO,), 0, NODE_DEV), jax.random.fold_in(seeds[5], 1), 0, NODE_DEV - 1).astype(jnp.int32)
    long_send = set_ends(jax.random.randint(seeds[6], (N_DOM, N_DOM, LONG_SLOT), 0, COARSE_DEV), jax.random.fold_in(seeds[6], 1), 0, COARSE_DEV - 1).astype(jnp.int32)
    edge_first = noise(seeds[7], (LAYERS, 3 * D, D), (3 * D) ** -0.5, 0.15625, ((2, 2),))
    edge_second = noise(seeds[8], (LAYERS, D, D), D ** -0.5, 0.25, ((2, 2),))
    node_first = noise(seeds[9], (LAYERS, 2 * D, D), (2 * D) ** -0.5, 0.1875, ((2, 2),))
    node_second = noise(seeds[10], (LAYERS, D, D), D ** -0.5, 0.25, ((2, 2),))
    edge_gain = jnp.clip(1.0 + 0.1 * jax.random.normal(seeds[11], (LAYERS, D), jnp.float32), 0.5, 1.5)
    edge_shift = noise(seeds[12], (LAYERS, D), 0.5, 3.0, (), jnp.float32)
    node_gain = jnp.clip(1.0 + 0.1 * jax.random.normal(seeds[13], (LAYERS, D), jnp.float32), 0.5, 1.5)
    node_shift = noise(seeds[14], (LAYERS, D), 0.5, 3.0, (), jnp.float32)
    return {"node_latents": node_latents, "edge_latents": edge_latents, "edge_senders": edge_senders, "edge_receivers": edge_receivers, "edge_counts": edge_counts, "halo_send": halo_send, "long_send": long_send, "edge_first": edge_first, "edge_second": edge_second, "node_first": node_first, "node_second": node_second, "edge_gain": edge_gain, "edge_shift": edge_shift, "node_gain": node_gain, "node_shift": node_shift}


def project_norm(inputs, first_weight, second, scale_gain, offset):
    hidden = jax.nn.silu(jnp.dot(inputs, first_weight, preferred_element_type=jnp.float32)).astype(jnp.bfloat16)
    output = jnp.dot(hidden, second, preferred_element_type=jnp.float32)
    average = lax.optimization_barrier(jnp.mean(output, -1, keepdims=True))
    centred = output - average
    variance = lax.optimization_barrier(jnp.mean(centred * centred, -1, keepdims=True))
    return centred * lax.rsqrt(variance + 1e-05) * scale_gain + offset

def reference(node_latents, edge_latents, edge_senders, edge_receivers, edge_counts, halo_send, long_send, edge_first, edge_second, node_first, node_second, edge_gain, edge_shift, node_gain, node_shift):
    partitions = N_DOM
    node_rows = NODE_DEV
    edge_rows = EDGE_DEV
    features = D
    members = node_latents.shape[0]
    halo_rows = halo_send.reshape(partitions, 2 * HALO)
    partition_ids = jnp.arange(partitions, dtype=jnp.int32)
    own_ids = partition_ids[:, None] * node_rows + jnp.arange(node_rows, dtype=jnp.int32)[None, :]
    previous = (partition_ids - 1) % partitions
    following = (partition_ids + 1) % partitions
    left_ids = previous[:, None] * node_rows + halo_rows[previous][:, HALO:]
    right_ids = following[:, None] * node_rows + halo_rows[following][:, :HALO]
    far_ids = partition_ids[None, :, None] * node_rows + jnp.transpose(long_send, (1, 0, 2))
    far_ids = far_ids.reshape(partitions, partitions * LONG_SLOT)
    source_ids = jnp.concatenate([own_ids, left_ids, right_ids, far_ids], 1).astype(jnp.int32)
    senders = edge_senders.reshape(partitions, edge_rows)
    sender_ids = jnp.take_along_axis(source_ids, senders, axis=1)
    receivers = edge_receivers.reshape(partitions, edge_rows)
    node_state = node_latents
    edge_state = jnp.transpose(edge_latents.reshape(members, partitions, edge_rows, features), (1, 0, 2, 3))
    for layer_index in range(LAYERS):

        def one_part(part_item):
            snd_ids, rcv_ids, live_count, edge_block, node_block = part_item
            sender_rows = jnp.take(node_state, snd_ids, axis=1)
            receiver_rows = jnp.take(node_block, rcv_ids, axis=1)
            joined = jnp.concatenate([edge_block, sender_rows, receiver_rows], -1).reshape(members * edge_rows, 3 * features)
            update = project_norm(joined, edge_first[layer_index], edge_second[layer_index], edge_gain[layer_index], edge_shift[layer_index]).reshape(members, edge_rows, features)
            live_mask = jnp.arange(edge_rows, dtype=jnp.int32) < live_count
            new_edges = jnp.where(live_mask[None, :, None], edge_block.astype(jnp.float32) + update, 0.0).astype(jnp.bfloat16)
            onehot = ((rcv_ids[None, :] == jnp.arange(node_rows, dtype=jnp.int32)[:, None]) & live_mask[None, :]).astype(jnp.float32)
            summed = jnp.einsum('ne,med->mnd', onehot, new_edges.astype(jnp.float32)).astype(jnp.bfloat16)
            node_in = jnp.concatenate([node_block, summed], -1).reshape(members * node_rows, 2 * features)
            node_update = project_norm(node_in, node_first[layer_index], node_second[layer_index], node_gain[layer_index], node_shift[layer_index]).reshape(members, node_rows, features)
            new_nodes = (node_block.astype(jnp.float32) + node_update).astype(jnp.bfloat16)
            return (new_nodes, new_edges)
        node_blocks = jnp.transpose(node_state.reshape(members, partitions, node_rows, features), (1, 0, 2, 3))
        new_nodes, new_edges = lax.map(one_part, (sender_ids, receivers, edge_counts, edge_state, node_blocks))
        node_state = jnp.transpose(new_nodes, (1, 0, 2, 3)).reshape(members, partitions * node_rows, features)
        edge_state = new_edges
    edge_final = jnp.transpose(edge_state, (1, 0, 2, 3)).reshape(members, partitions * edge_rows, features)
    return (node_state, edge_final)
```

```python
import functools

import jax
import jax.numpy as jnp
from jax import lax
from jax.experimental import pallas as pl
from jax.experimental.pallas import tpu as pltpu
from jax.sharding import PartitionSpec as P

F32, BF16 = jnp.float32, jnp.bfloat16
LANES = 128
CHUNK = 256


def round_up(value, step):
    return (value + step - 1) // step * step


def dot(a, b):
    return jnp.dot(a, b, preferred_element_type=F32)


def silu_of_half(half):
    return (half + half * jnp.tanh(half)).astype(BF16)


def norm(x, gain, shift):
    average = jnp.mean(x, -1, keepdims=True)
    centred = x - average
    variance = jnp.mean(centred * centred, -1, keepdims=True)
    return centred * lax.rsqrt(variance + 1e-05) * gain + shift


def wide_dot(x, w):
    return jnp.concatenate([dot(x, w[h]) for h in range(w.shape[0])], -1)


def edge_rows(m, c, refs):
    edge, pre, table, gather, w2, eg, eb, count, split = refs
    rows = slice(c * CHUNK, (c + 1) * CHUNK)
    hidden = jnp.concatenate(
        [silu_of_half(pre[h, m, rows, :] + dot(gather[rows, split:], table[h, m, split:, :])) for h in range(2)], -1
    )
    update = norm(wide_dot(hidden, w2), eg, eb)
    live = lax.broadcasted_iota(jnp.int32, (CHUNK, 1), 0) + c * CHUNK < count
    return rows, jnp.where(live, edge[m, rows, :].astype(F32) + update, 0.0).astype(BF16)


def node_rows(base, pre, summed, refs):
    w3b, w4, ng, nb = refs
    hidden = jnp.concatenate([silu_of_half(pre[h] + 0.5 * dot(summed, w3b[h])) for h in range(2)], -1)
    return (base.astype(F32) + norm(wide_dot(hidden, w4), ng, nb)).astype(BF16)


def exchange_kernel(
    sizes,
    node_in, edge_in, senders_in, receivers_in, counts_in, halo_in, long_in,
    ef_in, es_in, nf_in, ns_in, eg_in, eb_in, ng_in, nb_in,
    node, edge, pre, node_pre, table, gather, scatter, weights, norms, count_row,
    ids_v, count_s, halo_v, long_v, picked, picker, sent_scatter, sent, sent_pre, near, far_rows,
    halo_out, halo, far_out, far,
    node_sem, halo_sem, long_sem, ids_sem, count_sem, edge_sem, norm_sem,
    own_sem, ws_sem, wr_sem, hs_sem, hr_sem, fs_sem, fr_sem,
):
    n, layers, members, nodes, edges, width, side_rows, slots = sizes
    me = lax.axis_index("dom")
    core = lax.axis_index("mem")
    halves = 2
    other = 1 - core
    split = 2 * nodes
    near_rows = 2 * side_rows + n * slots
    everyone = range(members)

    barrier = pltpu.get_barrier_semaphore()
    pl.semaphore_signal(barrier, inc=1, device_id={"mem": other})
    for step in range(1, n):
        pl.semaphore_signal(barrier, inc=1, device_id={"dom": lax.rem(me + step, n)})

    def whole(ref, sem):
        return pltpu.make_async_copy(ref, ref, sem)

    blocks = ((ef_in, 0, 3), (es_in, 3, 1), (nf_in, 4, 2), (ns_in, 6, 1))

    def place(l, k, part):
        src, start, count = blocks[k]
        return src.at[l], weights.at[l, part, start * width : (start + count) * width]

    pltpu.make_async_copy(halo_in, halo_v, halo_sem).start()
    pltpu.make_async_copy(long_in.at[me], long_v, long_sem).start()
    pltpu.make_async_copy(node_in, node, node_sem).start()
    pltpu.make_async_copy(senders_in, ids_v.at[0], ids_sem).start()
    pltpu.make_async_copy(receivers_in, ids_v.at[1], ids_sem).start()
    pltpu.make_async_copy(counts_in, count_s, count_sem).start()
    pltpu.make_async_copy(*place(0, 0, core), own_sem.at[0, 0]).start()
    pltpu.make_async_copy(edge_in, edge, edge_sem).start()
    for k, src in enumerate((eg_in, eb_in, ng_in, nb_in)):
        pltpu.make_async_copy(src, norms.at[k], norm_sem).start()
    for l in range(layers):
        for k in range(4):
            if (l, k) != (0, 0):
                pltpu.make_async_copy(*place(l, k, core), own_sem.at[l, min(k, 1)]).start()

    def wait_weights(l, group):
        rows = weights.at[l, core, : 3 * width] if group == 0 else weights.at[l, core, 3 * width :]
        whole(rows, own_sem.at[l, group]).wait()

    def wait_partner(l, group):
        rows = weights.at[l, other, : 3 * width] if group == 0 else weights.at[l, other, 3 * width :]
        whole(rows, wr_sem.at[l, group]).wait()

    def column(row):
        wide = round_up(row.shape[1], LANES)
        if wide > row.shape[1]:
            row = jnp.concatenate([row, jnp.zeros((1, wide - row.shape[1]), jnp.int32)], 1)
        return jnp.transpose(jnp.broadcast_to(row, (LANES, wide)))

    def one_hot(hits):
        return hits.astype(F32).astype(BF16)

    whole(halo_v, halo_sem).wait()
    whole(long_v, long_sem).wait()
    picked[: 2 * side_rows, :] = column(halo_v[...].reshape(1, 2 * side_rows))[: 2 * side_rows]
    for s in range(slots):
        picked[pl.ds(2 * side_rows + s, n, stride=slots), :] = column(long_v[s : s + 1, :])[:n]
    for c in range(nodes // LANES):
        lane = lax.broadcasted_iota(jnp.int32, picked.shape, 1) + c * LANES
        picker[:, c * LANES : (c + 1) * LANES] = one_hot(picked[...] == lane)

    def stage(l, m, packed):
        for side in range(2):
            halo_out[l, m, side] = packed[side * side_rows : (side + 1) * side_rows]
        for q in range(n):
            start = 2 * side_rows + q * slots
            far_out[l, m, q] = packed[start : start + slots]

    def send(l, m):
        for step in range(1, n):
            target = lax.rem(me + step, n)
            pltpu.make_async_remote_copy(
                src_ref=far_out.at[l, m, target],
                dst_ref=far.at[l, m, me],
                send_sem=fs_sem.at[l, m],
                recv_sem=fr_sem.at[l, m],
                device_id={"dom": target},
            ).start()
        for side, step in ((1, 1), (0, n - 1)):
            pltpu.make_async_remote_copy(
                src_ref=halo_out.at[l, m, side],
                dst_ref=halo.at[l, m, 1 - side],
                send_sem=hs_sem.at[l, m],
                recv_sem=hr_sem.at[l, m],
                device_id={"dom": lax.rem(me + step, n)},
            ).start()
        pltpu.make_async_copy(far_out.at[l, m, me], far.at[l, m, me], fr_sem.at[l, m]).start()

    whole(node, node_sem).wait()
    for m in everyone:
        rows = dot(picker[...], node[m]).astype(BF16)
        sent[m] = rows
        stage(0, m, rows)
        if m == 0:
            pl.semaphore_wait(barrier, n)
        send(0, m)
    for l in range(layers):
        for k in range(4):
            src, dst = place(l, k, core)
            pltpu.make_async_remote_copy(
                src_ref=src,
                dst_ref=dst,
                send_sem=ws_sem.at[l],
                recv_sem=wr_sem.at[l, min(k, 1)],
                device_id={"mem": other},
            ).start()

    whole(ids_v, ids_sem).wait()
    depth = gather.shape[1]
    senders = column(ids_v[0:1, :])
    receiver_row = ids_v[1:2, :]
    receivers = column(receiver_row) + nodes
    senders = jnp.where(senders < nodes, senders, senders + nodes)
    for c in range(depth // LANES):
        lane = lax.broadcasted_iota(jnp.int32, (edges, LANES), 1) + c * LANES
        gather[:, c * LANES : (c + 1) * LANES] = one_hot((senders == lane) | (receivers == lane))
    row = lax.broadcasted_iota(jnp.int32, (nodes, edges), 0)
    scatter[...] = one_hot(jnp.broadcast_to(receiver_row, (nodes, edges)) == row)
    sent_scatter[...] = dot(picker[...], scatter[...]).astype(BF16)
    far_base = split + near_rows
    if far_base < depth:
        for h in range(halves):
            for m in everyone:
                table[h, m, far_base:, :] = jnp.zeros((depth - far_base, table.shape[3]), BF16)
    pltpu.make_async_copy(counts_in, count_s, count_sem).wait()
    count_row[...] = jnp.full(count_row.shape, count_s[0], jnp.int32)
    whole(edge, edge_sem).wait()
    whole(norms, norm_sem).wait()

    def prepare(l, h):
        w1 = weights.at[l, h]
        for m in everyone:
            table[h, m, :nodes, :] = (0.5 * dot(node[m], w1[width : 2 * width, :])).astype(BF16)
            table[h, m, nodes:split, :] = (0.5 * dot(node[m], w1[2 * width : 3 * width, :])).astype(BF16)
        for m in everyone:
            pre[h, m] = 0.5 * dot(edge[m], w1[:width, :]) + dot(gather[:, :split], table[h, m, :split, :])

    def node_prepare(l):
        for h in range(halves):
            w3a = weights[l, h, 4 * width : 5 * width, :]
            for m in everyone:
                if l < layers - 1:
                    sent_pre[m, h] = 0.5 * dot(sent[m], w3a)
                node_pre[m, h] = 0.5 * dot(node[m], w3a)

    def receive(l, ms):
        for m in ms:
            whole(far.at[l, m], fr_sem.at[l, m]).wait()
            whole(halo.at[l, m], hr_sem.at[l, m]).wait()
        for m in ms:
            for side in range(2):
                near[m, side * side_rows : (side + 1) * side_rows, :] = halo[l, m, side]
            for q in range(n):
                far_rows[m, q * slots : (q + 1) * slots, :] = far[l, m, q].astype(F32)
            near[m, 2 * side_rows :, :] = far_rows[m].astype(BF16)
            for h in range(halves):
                table[h, m, split : split + near_rows, :] = (
                    0.5 * dot(near[m], weights[l, h, width : 2 * width, :])
                ).astype(BF16)

    wait_weights(0, 0)
    prepare(0, core)
    wait_partner(0, 0)
    prepare(0, other)
    wait_weights(0, 1)
    wait_partner(0, 1)
    node_prepare(0)

    for l in range(layers):
        w = weights.at[l]
        receive(l, everyone)
        if l == layers - 1:
            continue
        node_refs = (
            w.at[:, 5 * width : 6 * width], w.at[:, 6 * width : 7 * width],
            norms[2, l : l + 1, :], norms[3, l : l + 1, :],
        )
        edge_refs = (
            edge, pre, table, gather, w.at[:, 3 * width : 4 * width],
            norms[0, l : l + 1, :], norms[1, l : l + 1, :], count_row[0:1, 0:1], split,
        )
        for c in range(edges // CHUNK):
            for m in everyone:
                rows, value = edge_rows(m, c, edge_refs)
                edge[m, rows, :] = value
        summed = jnp.concatenate([dot(sent_scatter[...], edge[m]).astype(BF16) for m in everyone], 0)
        base = jnp.concatenate([sent[m] for m in everyone], 0)
        started = [jnp.concatenate([sent_pre[m, h] for m in everyone], 0) for h in range(halves)]
        fresh = node_rows(base, started, summed, node_refs)
        for m in everyone:
            rows = fresh[m * near_rows : (m + 1) * near_rows]
            if l + 1 < layers - 1:
                sent[m] = rows
            stage(l + 1, m, rows)
            send(l + 1, m)
        for m in everyone:
            summed = dot(scatter[...], edge[m]).astype(BF16)
            node[m] = node_rows(node[m], [node_pre[m, h] for h in range(halves)], summed, node_refs)
        wait_weights(l + 1, 0)
        wait_partner(l + 1, 0)
        for h in range(halves):
            prepare(l + 1, h)
        wait_weights(l + 1, 1)
        wait_partner(l + 1, 1)
        node_prepare(l + 1)

    for l in range(layers):
        whole(weights.at[l, core], ws_sem.at[l]).wait()
        for m in everyone:
            whole(far_out.at[l, m, : n - 1], fs_sem.at[l, m]).wait()
            whole(halo_out.at[l, m], hs_sem.at[l, m]).wait()


def finish_kernel(
    sizes,
    node, edge, pre, node_pre, table, gather, scatter, weights, norms, count_row,
    node_out, edge_out, edge_new, node_new, sem,
):
    n, layers, members, nodes, edges, width, side_rows, slots = sizes
    l = layers - 1
    w = weights.at[l]
    copies = []

    def store(src, dst):
        copy = pltpu.make_async_copy(src, dst, sem.at[len(copies)])
        copy.start()
        copies.append(copy)

    everyone = range(members)
    halves = 2
    edge_refs = (
        edge, pre, table, gather, w.at[:, 3 * width : 4 * width],
        norms[0, l : l + 1, :], norms[1, l : l + 1, :], count_row[0:1, 0:1], 2 * nodes,
    )
    node_refs = (
        w.at[:, 5 * width : 6 * width], w.at[:, 6 * width : 7 * width],
        norms[2, l : l + 1, :], norms[3, l : l + 1, :],
    )
    for c in range(edges // CHUNK):
        for m in everyone:
            rows, value = edge_rows(m, c, edge_refs)
            edge_new[m, rows, :] = value
            store(edge_new.at[m, rows], edge_out.at[m, rows])
    summed = jnp.concatenate([dot(scatter[...], edge_new[m]).astype(BF16) for m in everyone], 0)
    base = jnp.concatenate([node[m] for m in everyone], 0)
    started = [jnp.concatenate([node_pre[m, h] for m in everyone], 0) for h in range(halves)]
    fresh = node_rows(base, started, summed, node_refs)
    for m in everyone:
        node_new[m] = fresh[m * nodes : (m + 1) * nodes]
    store(node_new, node_out)
    for copy in copies:
        copy.wait()


def solution(mesh):
    n = mesh.shape["dom"]

    def step(
        node, edge, senders, receivers, counts, halo_send, long_send, ef, es, nf, ns, eg, eb, ng, nb
    ):
        members, nodes, width = node.shape
        edges = edge.shape[1]
        layers = ef.shape[0]
        side_rows = halo_send.shape[0] // 2
        slots = long_send.shape[-1]
        long_rows = jnp.swapaxes(long_send, 1, 2)
        near_rows = 2 * side_rows + n * slots
        depth = 2 * nodes + round_up(near_rows, LANES)
        sizes = (n, layers, members, nodes, edges, width, side_rows, slots)
        half = width // 2
        hbm = pl.BlockSpec(memory_space=pltpu.HBM)
        vmem = pl.BlockSpec(memory_space=pltpu.VMEM)
        dma = pltpu.SemaphoreType.DMA
        kept = [
            (node.shape, BF16),
            (edge.shape, BF16),
            ((2, members, edges, half), F32),
            ((members, 2, nodes, half), F32),
            ((2, members, depth, half), BF16),
            ((edges, depth), BF16),
            ((nodes, edges), BF16),
            ((layers, 2, 7 * width, half), BF16),
            ((4,) + eg.shape, F32),
            ((1, LANES), jnp.int32),
        ]
        state = pl.pallas_call(
            functools.partial(exchange_kernel, sizes),
            out_shape=tuple(pltpu.VMEM(shape, kind) for shape, kind in kept),
            in_specs=[hbm] * 15,
            out_specs=(vmem,) * len(kept),
            scratch_shapes=[
                pltpu.VMEM((2,) + senders.shape, jnp.int32),
                pltpu.SMEM(counts.shape, jnp.int32),
                pltpu.VMEM(halo_send.shape, jnp.int32),
                pltpu.VMEM(long_rows.shape[1:], jnp.int32),
                pltpu.VMEM((near_rows, LANES), jnp.int32),
                pltpu.VMEM((near_rows, nodes), BF16),
                pltpu.VMEM((near_rows, edges), BF16),
                pltpu.VMEM((members, near_rows, width), BF16),
                pltpu.VMEM((members, 2, near_rows, half), F32),
                pltpu.VMEM((members, near_rows, width), BF16),
                pltpu.VMEM((members, n * slots, width), F32),
                pltpu.VMEM((layers, members, 2, side_rows, width), BF16),
                pltpu.VMEM((layers, members, 2, side_rows, width), BF16),
                pltpu.VMEM((layers, members, n, slots, width), BF16),
                pltpu.VMEM((layers, members, n, slots, width), BF16),
            ] + [dma(())] * 7 + [
                dma((layers, 2)),
                dma((layers,)),
                dma((layers, 2)),
                dma((layers, members)),
                dma((layers, members)),
                dma((layers, members)),
                dma((layers, members)),
            ],
            compiler_params=pltpu.CompilerParams(
                collective_id=0, has_side_effects=True, vmem_limit_bytes=51 * 1024 * 1024
            ),
        )(node, edge, senders, receivers, counts, halo_send, long_rows, ef, es, nf, ns, eg, eb, ng, nb)
        return pl.pallas_call(
            functools.partial(finish_kernel, sizes),
            out_shape=(
                jax.ShapeDtypeStruct(node.shape, BF16),
                jax.ShapeDtypeStruct(edge.shape, BF16),
            ),
            in_specs=[vmem] * len(kept),
            out_specs=(hbm, hbm),
            scratch_shapes=[
                pltpu.VMEM(edge.shape, BF16),
                pltpu.VMEM(node.shape, BF16),
                dma((1 + members * (edges // CHUNK),)),
            ],
            compiler_params=pltpu.CompilerParams(vmem_limit_bytes=40 * 1024 * 1024),
        )(*state)

    shared, halved = P(), P(None, None, "mem")
    parts = P("mem", "dom", None)
    placed = (parts,) * 2 + (P("dom"),) * 4 + (shared,) + (halved,) * 4 + (shared,) * 4
    return jax.shard_map(step, mesh=mesh, in_specs=placed, out_specs=(parts, parts), check_vma=False)
```

```python
import functools

import jax
import jax.numpy as jnp
from jax import lax
from jax.experimental import pallas as pl
from jax.experimental.pallas import tpu as pltpu
from jax.sharding import PartitionSpec as P

F32, BF16 = jnp.float32, jnp.bfloat16
LANES = 128
CHUNK = 256


def round_up(value, step):
    return (value + step - 1) // step * step


def dot(a, b):
    return jnp.dot(a, b, preferred_element_type=F32)


def silu_of_half(half):
    return (half + half * jnp.tanh(half)).astype(BF16)


def wide_dot(x, w):
    return jnp.concatenate([dot(x, w[h]) for h in range(w.shape[0])], -1)


def scaled(x, gain, live=None):
    factor = lax.rsqrt(jnp.mean(x * x, -1, keepdims=True) + 1e-05)
    if live is not None:
        factor = jnp.where(live, factor, 0.0)
    return x * factor * gain


def live_rows(start, rows, count):
    return lax.broadcasted_iota(jnp.int32, (rows, 1), 0) + start < count


def edge_rows(m, c, refs):
    base, pre, table, gather, w2, gain, count, split = refs
    rows = slice(c * CHUNK, (c + 1) * CHUNK)
    hidden = jnp.concatenate(
        [silu_of_half(pre[h, m, rows, :] + dot(gather[rows, split:], table[h, m, split:, :])) for h in range(2)], -1
    )
    update = scaled(wide_dot(hidden, w2), gain, live_rows(c * CHUNK, CHUNK, count))
    return rows, (base[m, rows, :] + update).astype(BF16)


def node_rows(base, pre, summed, refs):
    w3b, w4, gain = refs
    hidden = jnp.concatenate([silu_of_half(pre[h] + 0.5 * dot(summed, w3b[h])) for h in range(2)], -1)
    return (base + scaled(wide_dot(hidden, w4), gain)).astype(BF16)


def exchange_kernel(
    sizes,
    node_in, edge_in, senders_in, receivers_in, counts_in, halo_in, long_in,
    ef_in, es_in, nf_in, ns_in, eg_in, eb_in, ng_in, nb_in,
    node_base, edge_base, pre, node_pre, table, gather, scatter, weights, norms, count_row,
    node, edge, first, ids_v, count_s, halo_v, long_v, picked, picker, sent_scatter, sent, sent_base, sent_pre, near, far_rows,
    halo_out, halo, far_out, far,
    node_sem, halo_sem, long_sem, ids_sem, count_sem, edge_sem, norm_sem,
    own_sem, ws_sem, wr_sem, hs_sem, hr_sem, fs_sem, fr_sem,
):
    n, layers, members, nodes, edges, width, side_rows, slots = sizes
    me = lax.axis_index("dom")
    core = lax.axis_index("mem")
    halves = 2
    other = 1 - core
    split = 2 * nodes
    near_rows = 2 * side_rows + n * slots
    everyone = range(members)

    pltpu.make_async_copy(halo_in, halo_v, halo_sem).start()
    pltpu.make_async_copy(long_in.at[me], long_v, long_sem).start()
    pltpu.make_async_copy(node_in, node, node_sem).start()

    barrier = pltpu.get_barrier_semaphore()
    pl.semaphore_signal(barrier, inc=1, device_id={"mem": other})
    for step in range(1, n):
        pl.semaphore_signal(barrier, inc=1, device_id={"dom": lax.rem(me + step, n)})

    def whole(ref, sem):
        return pltpu.make_async_copy(ref, ref, sem)

    blocks = ((ef_in, 0, 3), (es_in, 0, 1), (nf_in, 1, 2), (ns_in, 3, 1))

    def place(l, k, part):
        src, start, count = blocks[k]
        held = weights if k else first
        return src.at[l], held.at[l, part, start * width : (start + count) * width]

    pltpu.make_async_copy(senders_in, ids_v.at[0], ids_sem).start()
    pltpu.make_async_copy(receivers_in, ids_v.at[1], ids_sem).start()
    pltpu.make_async_copy(counts_in, count_s, count_sem).start()
    pltpu.make_async_copy(*place(0, 0, core), own_sem.at[0, 0]).start()
    pltpu.make_async_copy(edge_in, edge, edge_sem).start()
    for k, src in enumerate((eg_in, eb_in, ng_in, nb_in)):
        pltpu.make_async_copy(src, norms.at[k], norm_sem).start()
    for l in range(layers):
        for k in range(4):
            if (l, k) != (0, 0):
                pltpu.make_async_copy(*place(l, k, core), own_sem.at[l, min(k, 1)]).start()

    def wait_weights(l, group):
        whole((weights if group else first).at[l, core], own_sem.at[l, group]).wait()

    def wait_partner(l, group):
        whole((weights if group else first).at[l, other], wr_sem.at[l, group]).wait()

    def column(row):
        wide = round_up(row.shape[1], LANES)
        if wide > row.shape[1]:
            row = jnp.concatenate([row, jnp.zeros((1, wide - row.shape[1]), jnp.int32)], 1)
        return jnp.transpose(jnp.broadcast_to(row, (LANES, wide)))

    def one_hot(hits):
        return hits.astype(F32).astype(BF16)

    whole(halo_v, halo_sem).wait()
    whole(long_v, long_sem).wait()
    picked[: 2 * side_rows, :] = column(halo_v[...].reshape(1, 2 * side_rows))[: 2 * side_rows]
    for s in range(slots):
        picked[pl.ds(2 * side_rows + s, n, stride=slots), :] = column(long_v[s : s + 1, :])[:n]
    for c in range(nodes // LANES):
        lane = lax.broadcasted_iota(jnp.int32, picked.shape, 1) + c * LANES
        picker[:, c * LANES : (c + 1) * LANES] = one_hot(picked[...] == lane)

    def stage(l, m, packed):
        for side in range(2):
            halo_out[l, side, m] = packed[side * side_rows : (side + 1) * side_rows]
        for q in range(n):
            start = 2 * side_rows + q * slots
            far_out[l, q, m] = packed[start : start + slots]

    def send(l):
        for side, step in ((1, 1), (0, n - 1)):
            pltpu.make_async_remote_copy(
                src_ref=halo_out.at[l, side],
                dst_ref=halo.at[l, 1 - side],
                send_sem=hs_sem.at[l],
                recv_sem=hr_sem.at[l],
                device_id={"dom": lax.rem(me + step, n)},
            ).start()
        for step in range(1, n):
            target = lax.rem(me + step, n)
            pltpu.make_async_remote_copy(
                src_ref=far_out.at[l, target],
                dst_ref=far.at[l, me],
                send_sem=fs_sem.at[l],
                recv_sem=fr_sem.at[l],
                device_id={"dom": target},
            ).start()
        pltpu.make_async_copy(far_out.at[l, me], far.at[l, me], fr_sem.at[l]).start()

    whole(node, node_sem).wait()
    for m in everyone:
        rows = dot(picker[...], node[m]).astype(BF16)
        sent[m] = rows
        stage(0, m, rows)
    pl.semaphore_wait(barrier, n)
    send(0)
    for l in range(layers):
        for k in range(4):
            src, dst = place(l, k, core)
            pltpu.make_async_remote_copy(
                src_ref=src,
                dst_ref=dst,
                send_sem=ws_sem.at[l, min(k, 1)],
                recv_sem=wr_sem.at[l, min(k, 1)],
                device_id={"mem": other},
            ).start()

    whole(ids_v, ids_sem).wait()
    depth = gather.shape[1]
    senders = column(ids_v[0:1, :])
    receiver_row = ids_v[1:2, :]
    receivers = column(receiver_row) + nodes
    senders = jnp.where(senders < nodes, senders, senders + nodes)
    for c in range(depth // LANES):
        lane = lax.broadcasted_iota(jnp.int32, (edges, LANES), 1) + c * LANES
        gather[:, c * LANES : (c + 1) * LANES] = one_hot((senders == lane) | (receivers == lane))
    row = lax.broadcasted_iota(jnp.int32, (nodes, edges), 0)
    scatter[...] = one_hot(jnp.broadcast_to(receiver_row, (nodes, edges)) == row)
    sent_scatter[...] = dot(picker[...], scatter[...]).astype(BF16)
    far_base = split + near_rows
    if far_base < depth:
        for h in range(halves):
            for m in everyone:
                table[h, m, far_base:, :] = jnp.zeros((depth - far_base, table.shape[3]), BF16)
    pltpu.make_async_copy(counts_in, count_s, count_sem).wait()
    count_row[...] = jnp.full(count_row.shape, count_s[0], jnp.int32)
    whole(edge, edge_sem).wait()
    whole(norms, norm_sem).wait()

    def prepare(l, h):
        w1 = first.at[l, h]
        for m in everyone:
            table[h, m, :nodes, :] = (0.5 * dot(node[m], w1[width : 2 * width, :])).astype(BF16)
            table[h, m, nodes:split, :] = (0.5 * dot(node[m], w1[2 * width : 3 * width, :])).astype(BF16)
        for m in everyone:
            pre[h, m] = 0.5 * dot(edge[m], w1[:width, :]) + dot(gather[:, :split], table[h, m, :split, :])

    def centre(l, start):
        for r in range(start, start + width, LANES):
            rows = slice(r, r + LANES)
            values = [weights[l, h, rows, :].astype(F32) for h in range(halves)]
            average = sum(jnp.sum(v, -1, keepdims=True) for v in values) / width
            for h in range(halves):
                weights[l, h, rows, :] = (values[h] - average).astype(BF16)

    def edge_prepare(l):
        for m in everyone:
            for r in range(0, edges, LANES):
                rows = slice(r, r + LANES)
                live = live_rows(r, LANES, count_row[0:1, 0:1])
                edge_base[m, rows, :] = jnp.where(live, edge[m, rows, :].astype(F32) + norms[1, l : l + 1, :], 0.0)

    def node_prepare(l):
        centre(l, 0)
        centre(l, 3 * width)
        for m in everyone:
            node_base[m] = node[m].astype(F32) + norms[3, l : l + 1, :]
            if l < layers - 1:
                sent_base[m * near_rows : (m + 1) * near_rows, :] = sent[m].astype(F32) + norms[3, l : l + 1, :]
        for h in range(halves):
            w3a = weights[l, h, width : 2 * width, :]
            for m in everyone:
                if l < layers - 1:
                    sent_pre[m, h] = 0.5 * dot(sent[m], w3a)
                node_pre[m, h] = 0.5 * dot(node[m], w3a)

    def receive(l, ms):
        whole(far.at[l], fr_sem.at[l]).wait()
        whole(halo.at[l], hr_sem.at[l]).wait()
        for m in ms:
            for side in range(2):
                near[m, side * side_rows : (side + 1) * side_rows, :] = halo[l, side, m]
            for q in range(n):
                far_rows[m, q * slots : (q + 1) * slots, :] = far[l, q, m].astype(F32)
            near[m, 2 * side_rows :, :] = far_rows[m].astype(BF16)
            for h in range(halves):
                table[h, m, split : split + near_rows, :] = (
                    0.5 * dot(near[m], first[l, h, width : 2 * width, :])
                ).astype(BF16)

    edge_prepare(0)
    wait_weights(0, 0)
    prepare(0, core)
    wait_partner(0, 0)
    prepare(0, other)
    wait_weights(0, 1)
    wait_partner(0, 1)
    node_prepare(0)

    for l in range(layers):
        w = weights.at[l]
        receive(l, everyone)
        if l == layers - 1:
            continue
        node_refs = (
            w.at[:, 2 * width : 3 * width], w.at[:, 3 * width :],
            norms[2, l : l + 1, :],
        )
        edge_refs = (
            edge_base, pre, table, gather, w.at[:, :width],
            norms[0, l : l + 1, :], count_row[0:1, 0:1], split,
        )
        for c in range(edges // CHUNK):
            for m in everyone:
                rows, value = edge_rows(m, c, edge_refs)
                edge[m, rows, :] = value
        summed = jnp.concatenate([dot(sent_scatter[...], edge[m]).astype(BF16) for m in everyone], 0)
        started = [jnp.concatenate([sent_pre[m, h] for m in everyone], 0) for h in range(halves)]
        fresh = node_rows(sent_base[...], started, summed, node_refs)
        for m in everyone:
            rows = fresh[m * near_rows : (m + 1) * near_rows]
            if l + 1 < layers - 1:
                sent[m] = rows
            stage(l + 1, m, rows)
        send(l + 1)
        for m in everyone:
            summed = dot(scatter[...], edge[m]).astype(BF16)
            node[m] = node_rows(node_base[m], [node_pre[m, h] for h in range(halves)], summed, node_refs)
        edge_prepare(l + 1)
        wait_weights(l + 1, 0)
        wait_partner(l + 1, 0)
        for h in range(halves):
            prepare(l + 1, h)
        wait_weights(l + 1, 1)
        wait_partner(l + 1, 1)
        node_prepare(l + 1)

    for l in range(layers):
        whole(first.at[l, core], ws_sem.at[l, 0]).wait()
        whole(weights.at[l, core], ws_sem.at[l, 1]).wait()
        whole(far_out.at[l, : n - 1], fs_sem.at[l]).wait()
        whole(halo_out.at[l], hs_sem.at[l]).wait()


def finish_kernel(
    sizes,
    node_base, edge_base, pre, node_pre, table, gather, scatter, weights, norms, count_row,
    node_out, edge_out, edge_new, node_new, sem,
):
    n, layers, members, nodes, edges, width, side_rows, slots = sizes
    l = layers - 1
    w = weights.at[l]
    copies = []

    def store(src, dst):
        copy = pltpu.make_async_copy(src, dst, sem.at[len(copies)])
        copy.start()
        copies.append(copy)

    everyone = range(members)
    halves = 2
    edge_refs = (
        edge_base, pre, table, gather, w.at[:, :width],
        norms[0, l : l + 1, :], count_row[0:1, 0:1], 2 * nodes,
    )
    node_refs = (
        w.at[:, 2 * width : 3 * width], w.at[:, 3 * width :],
        norms[2, l : l + 1, :],
    )
    for c in range(edges // CHUNK):
        for m in everyone:
            rows, value = edge_rows(m, c, edge_refs)
            edge_new[m, rows, :] = value
            store(edge_new.at[m, rows], edge_out.at[m, rows])
    summed = jnp.concatenate([dot(scatter[...], edge_new[m]).astype(BF16) for m in everyone], 0)
    base = jnp.concatenate([node_base[m] for m in everyone], 0)
    started = [jnp.concatenate([node_pre[m, h] for m in everyone], 0) for h in range(halves)]
    fresh = node_rows(base, started, summed, node_refs)
    for m in everyone:
        node_new[m] = fresh[m * nodes : (m + 1) * nodes]
    store(node_new, node_out)
    for copy in copies:
        copy.wait()


def solution(mesh):
    n = mesh.shape["dom"]

    def step(
        node, edge, senders, receivers, counts, halo_send, long_send, ef, es, nf, ns, eg, eb, ng, nb
    ):
        members, nodes, width = node.shape
        edges = edge.shape[1]
        layers = ef.shape[0]
        side_rows = halo_send.shape[0] // 2
        slots = long_send.shape[-1]
        long_rows = jnp.swapaxes(long_send, 1, 2)
        near_rows = 2 * side_rows + n * slots
        depth = 2 * nodes + round_up(near_rows, LANES)
        sizes = (n, layers, members, nodes, edges, width, side_rows, slots)
        half = width // 2
        hbm = pl.BlockSpec(memory_space=pltpu.HBM)
        vmem = pl.BlockSpec(memory_space=pltpu.VMEM)
        dma = pltpu.SemaphoreType.DMA
        kept = [
            (node.shape, F32),
            (edge.shape, F32),
            ((2, members, edges, half), F32),
            ((members, 2, nodes, half), F32),
            ((2, members, depth, half), BF16),
            ((edges, depth), BF16),
            ((nodes, edges), BF16),
            ((layers, 2, 4 * width, half), BF16),
            ((4,) + eg.shape, F32),
            ((1, LANES), jnp.int32),
        ]
        state = pl.pallas_call(
            functools.partial(exchange_kernel, sizes),
            out_shape=tuple(pltpu.VMEM(shape, kind) for shape, kind in kept),
            in_specs=[hbm] * 15,
            out_specs=(vmem,) * len(kept),
            scratch_shapes=[
                pltpu.VMEM(node.shape, BF16),
                pltpu.VMEM(edge.shape, BF16),
                pltpu.VMEM((layers, 2, ef.shape[1], half), BF16),
                pltpu.VMEM((2,) + senders.shape, jnp.int32),
                pltpu.SMEM(counts.shape, jnp.int32),
                pltpu.VMEM(halo_send.shape, jnp.int32),
                pltpu.VMEM(long_rows.shape[1:], jnp.int32),
                pltpu.VMEM((near_rows, LANES), jnp.int32),
                pltpu.VMEM((near_rows, nodes), BF16),
                pltpu.VMEM((near_rows, edges), BF16),
                pltpu.VMEM((members, near_rows, width), BF16),
                pltpu.VMEM((members * near_rows, width), F32),
                pltpu.VMEM((members, 2, near_rows, half), F32),
                pltpu.VMEM((members, near_rows, width), BF16),
                pltpu.VMEM((members, n * slots, width), F32),
                pltpu.VMEM((layers, 2, members, side_rows, width), BF16),
                pltpu.VMEM((layers, 2, members, side_rows, width), BF16),
                pltpu.VMEM((layers, n, members, slots, width), BF16),
                pltpu.VMEM((layers, n, members, slots, width), BF16),
            ] + [dma(())] * 7 + [
                dma((layers, 2)),
                dma((layers, 2)),
                dma((layers, 2)),
                dma((layers,)),
                dma((layers,)),
                dma((layers,)),
                dma((layers,)),
            ],
            compiler_params=pltpu.CompilerParams(
                collective_id=0, has_side_effects=True, vmem_limit_bytes=51 * 1024 * 1024
            ),
        )(node, edge, senders, receivers, counts, halo_send, long_rows, ef, es, nf, ns, eg, eb, ng, nb)
        return pl.pallas_call(
            functools.partial(finish_kernel, sizes),
            out_shape=(
                jax.ShapeDtypeStruct(node.shape, BF16),
                jax.ShapeDtypeStruct(edge.shape, BF16),
            ),
            in_specs=[vmem] * len(kept),
            out_specs=(hbm, hbm),
            scratch_shapes=[
                pltpu.VMEM(edge.shape, BF16),
                pltpu.VMEM(node.shape, BF16),
                dma((1 + members * (edges // CHUNK),)),
            ],
            compiler_params=pltpu.CompilerParams(vmem_limit_bytes=40 * 1024 * 1024),
        )(*state)

    shared, halved = P(), P(None, None, "mem")
    parts = P("mem", "dom", None)
    placed = (parts,) * 2 + (P("dom"),) * 4 + (shared,) + (halved,) * 4 + (shared,) * 4
    return jax.shard_map(step, mesh=mesh, in_specs=placed, out_specs=(parts, parts), check_vma=False)
```

```python
import functools

import jax
import jax.numpy as jnp
from jax import lax
from jax.experimental import pallas as pl
from jax.experimental.pallas import tpu as pltpu
from jax.sharding import PartitionSpec as P

F32, BF16 = jnp.float32, jnp.bfloat16
LANES = 128
CHUNK = 256


def round_up(value, step):
    return (value + step - 1) // step * step


def dot(a, b):
    return jnp.dot(a, b, preferred_element_type=F32)


def silu_of_half(half):
    return (half + half * jnp.tanh(half)).astype(BF16)


def wide_dot(x, w):
    return jnp.concatenate([dot(x, w[h]) for h in range(w.shape[0])], -1)


def scaled(x, gain):
    return x * lax.rsqrt(jnp.mean(x * x, -1, keepdims=True) + 1e-05) * gain


def live_rows(start, rows, count):
    return lax.broadcasted_iota(jnp.int32, (rows, 1), 0) + start < count


def node_chain(summed, base, pre, refs, finish):
    w3b, w4, gain = refs
    total = summed()
    yield
    hidden = jnp.concatenate([silu_of_half(pre(h) + 0.5 * dot(total, w3b[h])) for h in range(2)], -1)
    yield
    finish((base() + scaled(wide_dot(hidden, w4), gain)).astype(BF16))


def advance(chains):
    return [chain for chain in chains if next(chain, chain) is None]


def drain(chains):
    while chains:
        chains = advance(chains)


def edge_pass(members, edges, refs, write, chain_of):
    base, pre, table, gather, w2, gain, split = refs
    items = [(m, c) for m in range(members) for c in range(edges // CHUNK)]

    def hidden_of(m, c):
        rows = slice(c * CHUNK, (c + 1) * CHUNK)
        return jnp.concatenate(
            [silu_of_half(pre[h, m, rows, :] + dot(gather[rows, split:], table[h, m, split:, :])) for h in range(2)], -1
        )

    ahead = hidden_of(*items[0])
    chains = []
    for i, (m, c) in enumerate(items):
        hidden = ahead
        if i + 1 < len(items):
            ahead = hidden_of(*items[i + 1])
        rows = slice(c * CHUNK, (c + 1) * CHUNK)
        update = scaled(wide_dot(hidden, w2), gain)
        write(m, rows, (base[m, rows, :] + update).astype(BF16))
        chains = advance(chains)
        if (c + 1) * CHUNK == edges:
            chains.append(chain_of(m))
    drain(chains)


def exchange_kernel(
    sizes,
    node_in, edge_in, senders_in, receivers_in, counts_in, halo_in, long_in,
    ef_in, es_in, nf_in, ns_in, eg_in, eb_in, ng_in, nb_in,
    node_base, edge_base, pre, node_pre, table, gather, scatter, weights, norms,
    node, edge, first, ids_v, count_s, halo_v, long_v, picked, picker, sent_scatter, sent, sent_base, sent_pre, near,
    halo_out, halo, far_out, far,
    node_sem, halo_sem, long_sem, ids_sem, count_sem, edge_sem, norm_sem,
    own_sem, ws_sem, wr_sem, hs_sem, hr_sem, fs_sem, fr_sem,
):
    n, layers, members, nodes, edges, width, side_rows, slots = sizes
    me = lax.axis_index("dom")
    core = lax.axis_index("mem")
    halves = 2
    other = 1 - core
    split = 2 * nodes
    near_rows = 2 * side_rows + n * slots
    everyone = range(members)

    pltpu.make_async_copy(halo_in, halo_v, halo_sem).start()
    pltpu.make_async_copy(long_in.at[me], long_v, long_sem).start()
    pltpu.make_async_copy(node_in, node, node_sem).start()

    barrier = pltpu.get_barrier_semaphore()
    pl.semaphore_signal(barrier, inc=1, device_id={"mem": other})
    for step in range(1, n):
        pl.semaphore_signal(barrier, inc=1, device_id={"dom": lax.rem(me + step, n)})

    def whole(ref, sem):
        return pltpu.make_async_copy(ref, ref, sem)

    blocks = ((ef_in, 0, 3), (es_in, 0, 1), (nf_in, 1, 2), (ns_in, 3, 1))

    def place(l, k, part):
        src, start, count = blocks[k]
        held = weights if k else first
        return src.at[l], held.at[l, part, start * width : (start + count) * width]

    pltpu.make_async_copy(senders_in, ids_v.at[0], ids_sem).start()
    pltpu.make_async_copy(receivers_in, ids_v.at[1], ids_sem).start()
    pltpu.make_async_copy(counts_in, count_s, count_sem).start()
    pltpu.make_async_copy(*place(0, 0, core), own_sem.at[0, 0]).start()
    pltpu.make_async_copy(edge_in, edge, edge_sem).start()
    for k, src in enumerate((eg_in, eb_in, ng_in, nb_in)):
        pltpu.make_async_copy(src, norms.at[k], norm_sem).start()
    for l in range(layers):
        for k in range(4):
            if (l, k) != (0, 0):
                pltpu.make_async_copy(*place(l, k, core), own_sem.at[l, min(k, 1)]).start()

    def wait_weights(l, group):
        whole((weights if group else first).at[l, core], own_sem.at[l, group]).wait()

    def wait_partner(l, group):
        whole((weights if group else first).at[l, other], wr_sem.at[l, group]).wait()

    def column(row):
        wide = round_up(row.shape[1], LANES)
        if wide > row.shape[1]:
            row = jnp.concatenate([row, jnp.zeros((1, wide - row.shape[1]), jnp.int32)], 1)
        return jnp.transpose(jnp.broadcast_to(row, (LANES, wide)))

    def one_hot(hits):
        return hits.astype(F32).astype(BF16)

    whole(halo_v, halo_sem).wait()
    whole(long_v, long_sem).wait()
    picked[: 2 * side_rows, :] = column(halo_v[...].reshape(1, 2 * side_rows))[: 2 * side_rows]
    for s in range(slots):
        picked[pl.ds(2 * side_rows + s, n, stride=slots), :] = column(long_v[s : s + 1, :])[:n]
    for c in range(nodes // LANES):
        lane = lax.broadcasted_iota(jnp.int32, picked.shape, 1) + c * LANES
        picker[:, c * LANES : (c + 1) * LANES] = one_hot(picked[...] == lane)

    def stage(l, m, packed):
        for side in range(2):
            halo_out[l, side, m] = packed[side * side_rows : (side + 1) * side_rows]
        for q in range(n):
            start = 2 * side_rows + q * slots
            far_out[l, q, m] = packed[start : start + slots]

    def partner_of(mask):
        target, bit = 0, 1
        while bit < n:
            target = target + lax.rem(me // bit + (mask // bit) % 2, 2) * bit
            bit *= 2
        return target

    if n & (n - 1):
        targets = [lax.rem(me + step, n) for step in range(1, n)]
    else:
        targets = [partner_of(mask) for mask in range(n - 1, 0, -1)]

    def send_far(l, some):
        for target in some:
            pltpu.make_async_remote_copy(
                src_ref=far_out.at[l, target],
                dst_ref=far.at[l, me],
                send_sem=fs_sem.at[l],
                recv_sem=fr_sem.at[l],
                device_id={"dom": target},
            ).start()

    def send_halo(l):
        for side, step in ((0, n - 1), (1, 1)):
            pltpu.make_async_remote_copy(
                src_ref=halo_out.at[l, side],
                dst_ref=halo.at[l, 1 - side],
                send_sem=hs_sem.at[l],
                recv_sem=hr_sem.at[l],
                device_id={"dom": lax.rem(me + step, n)},
            ).start()

    def send(l):
        send_halo(l)
        send_far(l, targets)
        pltpu.make_async_copy(far_out.at[l, me], far.at[l, me], fr_sem.at[l]).start()

    whole(node, node_sem).wait()
    for m in everyone:
        rows = dot(picker[...], node[m]).astype(BF16)
        sent[m] = rows
        stage(0, m, rows)
    pl.semaphore_wait(barrier, n)
    send(0)
    for l in range(layers):
        for k in range(4):
            src, dst = place(l, k, core)
            pltpu.make_async_remote_copy(
                src_ref=src,
                dst_ref=dst,
                send_sem=ws_sem.at[l, min(k, 1)],
                recv_sem=wr_sem.at[l, min(k, 1)],
                device_id={"mem": other},
            ).start()

    whole(ids_v, ids_sem).wait()
    pltpu.make_async_copy(counts_in, count_s, count_sem).wait()
    count = count_s[0]
    depth = gather.shape[1]
    senders = column(ids_v[0:1, :])
    receiver_row = ids_v[1:2, :]
    receivers = column(receiver_row) + nodes
    senders = jnp.where(senders < nodes, senders, senders + nodes)
    for c in range(depth // LANES):
        lane = lax.broadcasted_iota(jnp.int32, (edges, LANES), 1) + c * LANES
        hits = ((senders == lane) | (receivers == lane)) & live_rows(0, edges, count)
        gather[:, c * LANES : (c + 1) * LANES] = one_hot(hits)
    row = lax.broadcasted_iota(jnp.int32, (nodes, edges), 0)
    scatter[...] = one_hot(jnp.broadcast_to(receiver_row, (nodes, edges)) == row)
    sent_scatter[...] = dot(picker[...], scatter[...]).astype(BF16)
    far_base = split + near_rows
    if far_base < depth:
        for h in range(halves):
            for m in everyone:
                table[h, m, far_base:, :] = jnp.zeros((depth - far_base, table.shape[3]), BF16)
    whole(edge, edge_sem).wait()
    whole(norms, norm_sem).wait()

    def prepare(l, h):
        w1 = first.at[l, h]
        for m in everyone:
            table[h, m, :nodes, :] = (0.5 * dot(node[m], w1[width : 2 * width, :])).astype(BF16)
            table[h, m, nodes:split, :] = (0.5 * dot(node[m], w1[2 * width : 3 * width, :])).astype(BF16)
        for m in everyone:
            pre[h, m] = 0.5 * dot(edge[m], w1[:width, :]) + dot(gather[:, :split], table[h, m, :split, :])

    def centre(l, start):
        for r in range(start, start + width, LANES):
            rows = slice(r, r + LANES)
            values = [weights[l, h, rows, :].astype(F32) for h in range(halves)]
            average = sum(jnp.sum(v, -1, keepdims=True) for v in values) / width
            for h in range(halves):
                weights[l, h, rows, :] = (values[h] - average).astype(BF16)

    def edge_prepare(l):
        for m in everyone:
            for r in range(0, edges, LANES):
                rows = slice(r, r + LANES)
                live = live_rows(r, LANES, count)
                kept = edge[m, rows, :].astype(F32)
                edge_base[m, rows, :] = jnp.where(live, kept + norms[1, l : l + 1, :], 0.0)
                if l == 0:
                    edge[m, rows, :] = jnp.where(live, kept, 0.0).astype(BF16)

    def node_prepare(l):
        centre(l, 0)
        centre(l, 3 * width)
        for m in everyone:
            node_base[m] = node[m].astype(F32) + norms[3, l : l + 1, :]
            if l < layers - 1:
                sent_base[m * near_rows : (m + 1) * near_rows, :] = sent[m].astype(F32) + norms[3, l : l + 1, :]
        for h in range(halves):
            w3a = weights[l, h, width : 2 * width, :]
            for m in everyone:
                if l < layers - 1:
                    sent_pre[m, h] = 0.5 * dot(sent[m], w3a)
                node_pre[m, h] = 0.5 * dot(node[m], w3a)

    def receive(l, ms):
        whole(far.at[l], fr_sem.at[l]).wait()
        whole(halo.at[l], hr_sem.at[l]).wait()
        for m in ms:
            for side in range(2):
                near[m, side * side_rows : (side + 1) * side_rows, :] = halo[l, side, m]
            near[m, 2 * side_rows :, :] = far[l, :, m].reshape(n * slots, width)
            for h in range(halves):
                table[h, m, split : split + near_rows, :] = (
                    0.5 * dot(near[m], first[l, h, width : 2 * width, :])
                ).astype(BF16)

    edge_prepare(0)
    wait_weights(0, 0)
    prepare(0, core)
    wait_partner(0, 0)
    prepare(0, other)
    wait_weights(0, 1)
    wait_partner(0, 1)
    node_prepare(0)

    for l in range(layers):
        w = weights.at[l]
        receive(l, everyone)
        if l == layers - 1:
            continue
        node_refs = (
            w.at[:, 2 * width : 3 * width], w.at[:, 3 * width :],
            norms[2, l : l + 1, :],
        )
        edge_refs = (
            edge_base, pre, table, gather, w.at[:, :width],
            norms[0, l : l + 1, :], split,
        )

        def write(m, rows, value):
            edge[m, rows, :] = value

        def sent_chain(m):
            rows = slice(m * near_rows, (m + 1) * near_rows)

            def finish(fresh):
                if l + 1 < layers - 1:
                    sent[m] = fresh
                stage(l + 1, m, fresh)

            return node_chain(
                lambda: dot(sent_scatter[...], edge[m]).astype(BF16),
                lambda: sent_base[rows, :], lambda h: sent_pre[m, h], node_refs, finish,
            )

        def kept_chain(m):
            def finish(fresh):
                node[m] = fresh

            return node_chain(
                lambda: dot(scatter[...], edge[m]).astype(BF16),
                lambda: node_base[m], lambda h: node_pre[m, h], node_refs, finish,
            )

        edge_pass(members, edges, edge_refs, write, sent_chain)
        send(l + 1)
        drain([kept_chain(m) for m in everyone])
        edge_prepare(l + 1)
        wait_weights(l + 1, 0)
        wait_partner(l + 1, 0)
        for h in range(halves):
            prepare(l + 1, h)
        wait_weights(l + 1, 1)
        wait_partner(l + 1, 1)
        node_prepare(l + 1)

    for l in range(layers):
        whole(first.at[l, core], ws_sem.at[l, 0]).wait()
        whole(weights.at[l, core], ws_sem.at[l, 1]).wait()
        whole(far_out.at[l, : n - 1], fs_sem.at[l]).wait()
        whole(halo_out.at[l], hs_sem.at[l]).wait()


def finish_kernel(
    sizes,
    node_base, edge_base, pre, node_pre, table, gather, scatter, weights, norms,
    node_out, edge_out, edge_new, node_new, sem,
):
    n, layers, members, nodes, edges, width, side_rows, slots = sizes
    l = layers - 1
    w = weights.at[l]
    copies = []

    def store(src, dst):
        copy = pltpu.make_async_copy(src, dst, sem.at[len(copies)])
        copy.start()
        copies.append(copy)

    edge_refs = (
        edge_base, pre, table, gather, w.at[:, :width],
        norms[0, l : l + 1, :], 2 * nodes,
    )
    node_refs = (
        w.at[:, 2 * width : 3 * width], w.at[:, 3 * width :],
        norms[2, l : l + 1, :],
    )

    def write(m, rows, value):
        edge_new[m, rows, :] = value
        store(edge_new.at[m, rows], edge_out.at[m, rows])

    def chain_of(m):
        def finish(fresh):
            node_new[m] = fresh
            store(node_new.at[m], node_out.at[m])

        return node_chain(
            lambda: dot(scatter[...], edge_new[m]).astype(BF16),
            lambda: node_base[m], lambda h: node_pre[m, h], node_refs, finish,
        )

    edge_pass(members, edges, edge_refs, write, chain_of)
    for copy in copies:
        copy.wait()


def solution(mesh):
    n = mesh.shape["dom"]

    def step(
        node, edge, senders, receivers, counts, halo_send, long_send, ef, es, nf, ns, eg, eb, ng, nb
    ):
        members, nodes, width = node.shape
        edges = edge.shape[1]
        layers = ef.shape[0]
        side_rows = halo_send.shape[0] // 2
        slots = long_send.shape[-1]
        long_rows = jnp.swapaxes(long_send, 1, 2)
        near_rows = 2 * side_rows + n * slots
        depth = 2 * nodes + round_up(near_rows, LANES)
        sizes = (n, layers, members, nodes, edges, width, side_rows, slots)
        half = width // 2
        hbm = pl.BlockSpec(memory_space=pltpu.HBM)
        vmem = pl.BlockSpec(memory_space=pltpu.VMEM)
        dma = pltpu.SemaphoreType.DMA
        kept = [
            (node.shape, F32),
            (edge.shape, F32),
            ((2, members, edges, half), F32),
            ((members, 2, nodes, half), F32),
            ((2, members, depth, half), BF16),
            ((edges, depth), BF16),
            ((nodes, edges), BF16),
            ((layers, 2, 4 * width, half), BF16),
            ((4,) + eg.shape, F32),
        ]
        state = pl.pallas_call(
            functools.partial(exchange_kernel, sizes),
            out_shape=tuple(pltpu.VMEM(shape, kind) for shape, kind in kept),
            in_specs=[hbm] * 15,
            out_specs=(vmem,) * len(kept),
            scratch_shapes=[
                pltpu.VMEM(node.shape, BF16),
                pltpu.VMEM(edge.shape, BF16),
                pltpu.VMEM((layers, 2, ef.shape[1], half), BF16),
                pltpu.VMEM((2,) + senders.shape, jnp.int32),
                pltpu.SMEM(counts.shape, jnp.int32),
                pltpu.VMEM(halo_send.shape, jnp.int32),
                pltpu.VMEM(long_rows.shape[1:], jnp.int32),
                pltpu.VMEM((near_rows, LANES), jnp.int32),
                pltpu.VMEM((near_rows, nodes), BF16),
                pltpu.VMEM((near_rows, edges), BF16),
                pltpu.VMEM((members, near_rows, width), BF16),
                pltpu.VMEM((members * near_rows, width), F32),
                pltpu.VMEM((members, 2, near_rows, half), F32),
                pltpu.VMEM((members, near_rows, width), BF16),
                pltpu.VMEM((layers, 2, members, side_rows, width), BF16),
                pltpu.VMEM((layers, 2, members, side_rows, width), BF16),
                pltpu.VMEM((layers, n, members, slots, width), BF16),
                pltpu.VMEM((layers, n, members, slots, width), BF16),
            ] + [dma(())] * 7 + [
                dma((layers, 2)),
                dma((layers, 2)),
                dma((layers, 2)),
                dma((layers,)),
                dma((layers,)),
                dma((layers,)),
                dma((layers,)),
            ],
            compiler_params=pltpu.CompilerParams(
                collective_id=0, has_side_effects=True, vmem_limit_bytes=51 * 1024 * 1024
            ),
        )(node, edge, senders, receivers, counts, halo_send, long_rows, ef, es, nf, ns, eg, eb, ng, nb)
        return pl.pallas_call(
            functools.partial(finish_kernel, sizes),
            out_shape=(
                jax.ShapeDtypeStruct(node.shape, BF16),
                jax.ShapeDtypeStruct(edge.shape, BF16),
            ),
            in_specs=[vmem] * len(kept),
            out_specs=(hbm, hbm),
            scratch_shapes=[
                pltpu.VMEM(edge.shape, BF16),
                pltpu.VMEM(node.shape, BF16),
                dma((members * (1 + edges // CHUNK),)),
            ],
            compiler_params=pltpu.CompilerParams(vmem_limit_bytes=40 * 1024 * 1024),
        )(*state)

    shared, halved = P(), P(None, None, "mem")
    parts = P("mem", "dom", None)
    placed = (parts,) * 2 + (P("dom"),) * 4 + (shared,) + (halved,) * 4 + (shared,) * 4
    return jax.shard_map(step, mesh=mesh, in_specs=placed, out_specs=(parts, parts), check_vma=False)
```

```python
import functools

import jax
import jax.numpy as jnp
from jax import lax
from jax.experimental import pallas as pl
from jax.experimental.pallas import tpu as pltpu
from jax.sharding import PartitionSpec as P

F32, BF16 = jnp.float32, jnp.bfloat16
LANES = 128
CHUNK = 256


def round_up(value, step):
    return (value + step - 1) // step * step


def dot(a, b):
    return jnp.dot(a, b, preferred_element_type=F32)


def silu_of_half(half):
    return (half + half * jnp.tanh(half)).astype(BF16)


def wide_dot(x, w):
    return jnp.concatenate([dot(x, w[h]) for h in range(w.shape[0])], -1)


def scaled(x, gain):
    return x * lax.rsqrt(jnp.mean(x * x, -1, keepdims=True) + 1e-05) * gain


def live_rows(start, rows, count):
    return lax.broadcasted_iota(jnp.int32, (rows, 1), 0) + start < count


def node_chain(summed, base, pre, refs, finish):
    w3b, w4, gain = refs
    total = summed()
    yield
    hidden = jnp.concatenate([silu_of_half(pre(h) + 0.5 * dot(total, w3b[h])) for h in range(2)], -1)
    yield
    finish((base() + scaled(wide_dot(hidden, w4), gain)).astype(BF16))


def advance(chains):
    return [chain for chain in chains if next(chain, chain) is None]


def drain(chains):
    while chains:
        chains = advance(chains)


def edge_pass(members, edges, refs, write, chain_of):
    base, pre, table, gather, w2, gain, split = refs
    items = [(m, c) for m in range(members) for c in range(edges // CHUNK)]

    def hidden_of(m, c):
        rows = slice(c * CHUNK, (c + 1) * CHUNK)
        return jnp.concatenate(
            [silu_of_half(pre[h, m, rows, :] + dot(gather[rows, split:], table[h, m, split:, :])) for h in range(2)], -1
        )

    ahead = hidden_of(*items[0])
    chains = []
    for i, (m, c) in enumerate(items):
        hidden = ahead
        if i + 1 < len(items):
            ahead = hidden_of(*items[i + 1])
        rows = slice(c * CHUNK, (c + 1) * CHUNK)
        update = scaled(wide_dot(hidden, w2), gain)
        write(m, rows, (base[m, rows, :] + update).astype(BF16))
        chains = advance(chains)
        if (c + 1) * CHUNK == edges:
            chains.append(chain_of(m))
    drain(chains)


def exchange_body(
    sizes,
    node_in, edge_in, senders_in, receivers_in, counts_in, halo_in, long_in,
    ef_in, es_in, nf_in, ns_in, eg_in, eb_in, ng_in, nb_in,
    node_base, edge_base, pre, node_pre, table, gather, scatter, weights, norms,
    node, edge, first, ids_v, count_s, halo_v, long_v, picked, picker, sent_scatter, sent, sent_base, sent_pre,
    outgoing, incoming,
    wr_sem, in_sem,
    node_sem, halo_sem, long_sem, ids_sem, count_sem, edge_sem, norm_sem, own_sem, ws_sem, out_sem,
):
    n, layers, members, nodes, edges, width, side_rows, slots = sizes
    me = lax.axis_index("dom")
    core = lax.axis_index("mem")
    halves = 2
    other = 1 - core
    split = 2 * nodes
    near_rows = 2 * side_rows + n * slots
    everyone = range(members)

    pltpu.make_async_copy(halo_in, halo_v, halo_sem).start()
    pltpu.make_async_copy(long_in.at[me], long_v, long_sem).start()
    pltpu.make_async_copy(node_in, node, node_sem).start()

    barrier = pltpu.get_barrier_semaphore()
    pl.semaphore_signal(barrier, inc=1, device_id={"mem": other})
    for step in range(1, n):
        pl.semaphore_signal(barrier, inc=1, device_id={"dom": lax.rem(me + step, n)})

    def whole(ref, sem):
        return pltpu.make_async_copy(ref, ref, sem)

    blocks = ((ef_in, 0, 3), (es_in, 0, 1), (nf_in, 1, 2), (ns_in, 3, 1))

    def place(l, k, part):
        src, start, count = blocks[k]
        held = weights if k else first
        return src.at[l], held.at[l, part, start * width : (start + count) * width]

    pltpu.make_async_copy(senders_in, ids_v.at[0], ids_sem).start()
    pltpu.make_async_copy(receivers_in, ids_v.at[1], ids_sem).start()
    pltpu.make_async_copy(counts_in, count_s, count_sem).start()
    pltpu.make_async_copy(*place(0, 0, core), own_sem.at[0, 0]).start()
    pltpu.make_async_copy(edge_in, edge, edge_sem).start()
    for k, src in enumerate((eg_in, eb_in, ng_in, nb_in)):
        pltpu.make_async_copy(src, norms.at[k], norm_sem).start()
    for l in range(layers):
        for k in range(4):
            if (l, k) != (0, 0):
                pltpu.make_async_copy(*place(l, k, core), own_sem.at[l, min(k, 1)]).start()

    def wait_weights(l, group):
        whole((weights if group else first).at[l, core], own_sem.at[l, group]).wait()

    def wait_partner(l, group):
        whole((weights if group else first).at[l, other], wr_sem.at[l, group]).wait()

    def column(row):
        wide = round_up(row.shape[1], LANES)
        if wide > row.shape[1]:
            row = jnp.concatenate([row, jnp.zeros((1, wide - row.shape[1]), jnp.int32)], 1)
        return jnp.transpose(jnp.broadcast_to(row, (LANES, wide)))

    def one_hot(hits):
        return hits.astype(F32).astype(BF16)

    whole(halo_v, halo_sem).wait()
    whole(long_v, long_sem).wait()
    picked[: 2 * side_rows, :] = column(halo_v[...].reshape(1, 2 * side_rows))[: 2 * side_rows]
    for s in range(slots):
        picked[pl.ds(2 * side_rows + s, n, stride=slots), :] = column(long_v[s : s + 1, :])[:n]
    for c in range(nodes // LANES):
        lane = lax.broadcasted_iota(jnp.int32, picked.shape, 1) + c * LANES
        picker[:, c * LANES : (c + 1) * LANES] = one_hot(picked[...] == lane)

    span = side_rows // slots

    def stage(l, m, packed):
        outgoing[l, :, m] = packed.reshape(2 * span + n, slots, width)

    def partner_of(mask):
        target, bit = 0, 1
        while bit < n:
            target = target + lax.rem(me // bit + (mask // bit) % 2, 2) * bit
            bit *= 2
        return target

    if n & (n - 1):
        targets = [lax.rem(me + step, n) for step in range(1, n)]
    else:
        targets = [partner_of(mask) for mask in range(n - 1, 0, -1)]

    def send(l):
        pieces = [(side * span, (1 - side) * span, span, lax.rem(me + step, n)) for side, step in ((0, n - 1), (1, 1))]
        pieces += [(2 * span + target, 2 * span + me, 1, target) for target in targets]
        pieces = pieces[2:3] + pieces[:2] + pieces[3:]
        for start, landing, count, target in pieces:
            pltpu.make_async_remote_copy(
                src_ref=outgoing.at[l, pl.ds(start, count)],
                dst_ref=incoming.at[l, pl.ds(landing, count)],
                send_sem=out_sem.at[l],
                recv_sem=in_sem.at[l],
                device_id={"dom": target},
            ).start()
        mine = pl.ds(2 * span + me, 1)
        pltpu.make_async_copy(outgoing.at[l, mine], incoming.at[l, mine], in_sem.at[l]).start()

    whole(node, node_sem).wait()
    for m in everyone:
        rows = dot(picker[...], node[m]).astype(BF16)
        sent[m] = rows
        stage(0, m, rows)
    pl.semaphore_wait(barrier, n)
    send(0)
    for l in range(layers):
        for k in range(4):
            src, dst = place(l, k, core)
            pltpu.make_async_remote_copy(
                src_ref=src,
                dst_ref=dst,
                send_sem=ws_sem.at[min(k, 1)],
                recv_sem=wr_sem.at[l, min(k, 1)],
                device_id={"mem": other},
            ).start()

    whole(ids_v, ids_sem).wait()
    pltpu.make_async_copy(counts_in, count_s, count_sem).wait()
    count = count_s[0]
    depth = gather.shape[1]
    senders = column(ids_v[0:1, :])
    receiver_row = ids_v[1:2, :]
    receivers = column(receiver_row) + nodes
    senders = jnp.where(senders < nodes, senders, senders + nodes)
    for c in range(depth // LANES):
        lane = lax.broadcasted_iota(jnp.int32, (edges, LANES), 1) + c * LANES
        hits = ((senders == lane) | (receivers == lane)) & live_rows(0, edges, count)
        gather[:, c * LANES : (c + 1) * LANES] = one_hot(hits)
    row = lax.broadcasted_iota(jnp.int32, (nodes, edges), 0)
    scatter[...] = one_hot(jnp.broadcast_to(receiver_row, (nodes, edges)) == row)
    sent_scatter[...] = dot(picker[...], scatter[...]).astype(BF16)
    far_base = split + near_rows
    if far_base < depth:
        for h in range(halves):
            for m in everyone:
                table[h, m, far_base:, :] = jnp.zeros((depth - far_base, table.shape[3]), BF16)
    whole(edge, edge_sem).wait()
    whole(norms, norm_sem).wait()

    def prepare(l, h):
        w1 = first.at[l, h]
        for m in everyone:
            table[h, m, :nodes, :] = (0.5 * dot(node[m], w1[width : 2 * width, :])).astype(BF16)
            table[h, m, nodes:split, :] = (0.5 * dot(node[m], w1[2 * width : 3 * width, :])).astype(BF16)
        for m in everyone:
            pre[h, m] = 0.5 * dot(edge[m], w1[:width, :]) + dot(gather[:, :split], table[h, m, :split, :])

    def centre(l, start):
        for r in range(start, start + width, LANES):
            rows = slice(r, r + LANES)
            values = [weights[l, h, rows, :].astype(F32) for h in range(halves)]
            average = sum(jnp.sum(v, -1, keepdims=True) for v in values) / width
            for h in range(halves):
                weights[l, h, rows, :] = (values[h] - average).astype(BF16)

    def edge_prepare(l):
        for m in everyone:
            for r in range(0, edges, LANES):
                rows = slice(r, r + LANES)
                live = live_rows(r, LANES, count)
                kept = edge[m, rows, :].astype(F32)
                edge_base[m, rows, :] = jnp.where(live, kept + norms[1, l : l + 1, :], 0.0)
                if l == 0:
                    edge[m, rows, :] = jnp.where(live, kept, 0.0).astype(BF16)

    def node_prepare(l):
        centre(l, 0)
        centre(l, 3 * width)
        for m in everyone:
            node_base[m] = node[m].astype(F32) + norms[3, l : l + 1, :]
            if l < layers - 1:
                sent_base[m * near_rows : (m + 1) * near_rows, :] = sent[m].astype(F32) + norms[3, l : l + 1, :]
        for h in range(halves):
            w3a = weights[l, h, width : 2 * width, :]
            for m in everyone:
                if l < layers - 1:
                    sent_pre[m, h] = 0.5 * dot(sent[m], w3a)
                node_pre[m, h] = 0.5 * dot(node[m], w3a)

    def receive(l, ms):
        whole(incoming.at[l], in_sem.at[l]).wait()
        for m in ms:
            near = incoming[l, :, m].reshape(near_rows, width)
            for h in range(halves):
                table[h, m, split : split + near_rows, :] = (
                    0.5 * dot(near, first[l, h, width : 2 * width, :])
                ).astype(BF16)

    edge_prepare(0)
    wait_weights(0, 0)
    prepare(0, core)
    wait_partner(0, 0)
    prepare(0, other)
    wait_weights(0, 1)
    wait_partner(0, 1)
    node_prepare(0)

    for l in range(layers):
        w = weights.at[l]
        receive(l, everyone)
        if l == layers - 1:
            continue
        node_refs = (
            w.at[:, 2 * width : 3 * width], w.at[:, 3 * width :],
            norms[2, l : l + 1, :],
        )
        edge_refs = (
            edge_base, pre, table, gather, w.at[:, :width],
            norms[0, l : l + 1, :], split,
        )

        def write(m, rows, value):
            edge[m, rows, :] = value

        def sent_chain(m):
            rows = slice(m * near_rows, (m + 1) * near_rows)

            def finish(fresh):
                if l + 1 < layers - 1:
                    sent[m] = fresh
                stage(l + 1, m, fresh)

            return node_chain(
                lambda: dot(sent_scatter[...], edge[m]).astype(BF16),
                lambda: sent_base[rows, :], lambda h: sent_pre[m, h], node_refs, finish,
            )

        def kept_chain(m):
            def finish(fresh):
                node[m] = fresh

            return node_chain(
                lambda: dot(scatter[...], edge[m]).astype(BF16),
                lambda: node_base[m], lambda h: node_pre[m, h], node_refs, finish,
            )

        edge_pass(members, edges, edge_refs, write, sent_chain)
        send(l + 1)
        drain([kept_chain(m) for m in everyone])
        edge_prepare(l + 1)
        wait_weights(l + 1, 0)
        wait_partner(l + 1, 0)
        for h in range(halves):
            prepare(l + 1, h)
        wait_weights(l + 1, 1)
        wait_partner(l + 1, 1)
        node_prepare(l + 1)

    whole(first.at[:, core], ws_sem.at[0]).wait()
    whole(weights.at[:, core], ws_sem.at[1]).wait()
    for l in range(layers):
        whole(outgoing.at[l, : 2 * span + n - 1], out_sem.at[l]).wait()


def exchange_kernel(sizes, *refs):
    layers, dma = sizes[1], pltpu.SemaphoreType.DMA
    local = [dma(())] * 7 + [dma((layers, 2)), dma((2,)), dma((layers,))]
    pl.run_scoped(functools.partial(exchange_body, sizes, *refs), *local)


def finish_body(
    sizes,
    node_base, edge_base, pre, node_pre, table, gather, scatter, weights, norms,
    node_out, edge_out, edge_new, node_new, edge_sem, node_sem,
):
    n, layers, members, nodes, edges, width, side_rows, slots = sizes
    l = layers - 1
    w = weights.at[l]
    edge_refs = (
        edge_base, pre, table, gather, w.at[:, :width],
        norms[0, l : l + 1, :], 2 * nodes,
    )
    node_refs = (
        w.at[:, 2 * width : 3 * width], w.at[:, 3 * width :],
        norms[2, l : l + 1, :],
    )

    def write(m, rows, value):
        edge_new[m, rows, :] = value
        pltpu.make_async_copy(edge_new.at[m, rows], edge_out.at[m, rows], edge_sem).start()

    def chain_of(m):
        def finish(fresh):
            node_new[m] = fresh
            pltpu.make_async_copy(node_new.at[m], node_out.at[m], node_sem).start()

        return node_chain(
            lambda: dot(scatter[...], edge_new[m]).astype(BF16),
            lambda: node_base[m], lambda h: node_pre[m, h], node_refs, finish,
        )

    edge_pass(members, edges, edge_refs, write, chain_of)
    pltpu.make_async_copy(edge_new, edge_out, edge_sem).wait()
    pltpu.make_async_copy(node_new, node_out, node_sem).wait()


def finish_kernel(sizes, *refs):
    dma = pltpu.SemaphoreType.DMA
    pl.run_scoped(functools.partial(finish_body, sizes, *refs), dma(()), dma(()))


def solution(mesh):
    n = mesh.shape["dom"]

    def step(
        node, edge, senders, receivers, counts, halo_send, long_send, ef, es, nf, ns, eg, eb, ng, nb
    ):
        members, nodes, width = node.shape
        edges = edge.shape[1]
        layers = ef.shape[0]
        side_rows = halo_send.shape[0] // 2
        slots = long_send.shape[-1]
        long_rows = jnp.swapaxes(long_send, 1, 2)
        near_rows = 2 * side_rows + n * slots
        depth = 2 * nodes + round_up(near_rows, LANES)
        sizes = (n, layers, members, nodes, edges, width, side_rows, slots)
        half = width // 2
        hbm = pl.BlockSpec(memory_space=pltpu.HBM)
        vmem = pl.BlockSpec(memory_space=pltpu.VMEM)
        dma = pltpu.SemaphoreType.DMA
        kept = [
            (node.shape, F32),
            (edge.shape, F32),
            ((2, members, edges, half), F32),
            ((members, 2, nodes, half), F32),
            ((2, members, depth, half), BF16),
            ((edges, depth), BF16),
            ((nodes, edges), BF16),
            ((layers, 2, 4 * width, half), BF16),
            ((4,) + eg.shape, F32),
        ]
        state = pl.pallas_call(
            functools.partial(exchange_kernel, sizes),
            out_shape=tuple(pltpu.VMEM(shape, kind) for shape, kind in kept),
            in_specs=[hbm] * 15,
            out_specs=(vmem,) * len(kept),
            scratch_shapes=[
                pltpu.VMEM(node.shape, BF16),
                pltpu.VMEM(edge.shape, BF16),
                pltpu.VMEM((layers, 2, ef.shape[1], half), BF16),
                pltpu.VMEM((2,) + senders.shape, jnp.int32),
                pltpu.SMEM(counts.shape, jnp.int32),
                pltpu.VMEM(halo_send.shape, jnp.int32),
                pltpu.VMEM(long_rows.shape[1:], jnp.int32),
                pltpu.VMEM((near_rows, LANES), jnp.int32),
                pltpu.VMEM((near_rows, nodes), BF16),
                pltpu.VMEM((near_rows, edges), BF16),
                pltpu.VMEM((members, near_rows, width), BF16),
                pltpu.VMEM((members * near_rows, width), F32),
                pltpu.VMEM((members, 2, near_rows, half), F32),
                pltpu.VMEM((layers, near_rows // slots, members, slots, width), BF16),
                pltpu.VMEM((layers, near_rows // slots, members, slots, width), BF16),
                dma((layers, 2)),
                dma((layers,)),
            ],
            compiler_params=pltpu.CompilerParams(
                collective_id=0, has_side_effects=True, vmem_limit_bytes=51 * 1024 * 1024
            ),
        )(node, edge, senders, receivers, counts, halo_send, long_rows, ef, es, nf, ns, eg, eb, ng, nb)
        return pl.pallas_call(
            functools.partial(finish_kernel, sizes),
            out_shape=(
                jax.ShapeDtypeStruct(node.shape, BF16),
                jax.ShapeDtypeStruct(edge.shape, BF16),
            ),
            in_specs=[vmem] * len(kept),
            out_specs=(hbm, hbm),
            scratch_shapes=[
                pltpu.VMEM(edge.shape, BF16),
                pltpu.VMEM(node.shape, BF16),
            ],
            compiler_params=pltpu.CompilerParams(vmem_limit_bytes=40 * 1024 * 1024),
        )(*state)

    shared, halved = P(), P(None, None, "mem")
    parts = P("mem", "dom", None)
    placed = (parts,) * 2 + (P("dom"),) * 4 + (shared,) + (halved,) * 4 + (shared,) * 4
    return jax.shard_map(step, mesh=mesh, in_specs=placed, out_specs=(parts, parts), check_vma=False)
```

```python
import functools

import jax
import jax.numpy as jnp
from jax import lax
from jax.experimental import pallas as pl
from jax.experimental.pallas import tpu as pltpu
from jax.sharding import PartitionSpec as P

F32, BF16 = jnp.float32, jnp.bfloat16
LANES = 128
CHUNK = 256


def round_up(value, step):
    return (value + step - 1) // step * step


def dot(a, b):
    return jnp.dot(a, b, preferred_element_type=F32)


def silu_of_half(half):
    return (half + half * jnp.tanh(half)).astype(BF16)


def wide_dot(x, w):
    return jnp.concatenate([dot(x, w[h]) for h in range(w.shape[0])], -1)


def scaled(x, gain):
    return x * lax.rsqrt(jnp.mean(x * x, -1, keepdims=True) + 1e-05) * gain


def live_rows(start, rows, count):
    return lax.broadcasted_iota(jnp.int32, (rows, 1), 0) + start < count


def node_chain(summed, base, pre, refs, finish):
    w3b, w4, gain = refs
    total = summed()
    yield
    hidden = jnp.concatenate([silu_of_half(pre(h) + 0.5 * dot(total, w3b[h])) for h in range(2)], -1)
    yield
    finish((base() + scaled(wide_dot(hidden, w4), gain)).astype(BF16))


def advance(chains):
    return [chain for chain in chains if next(chain, chain) is None]


def drain(chains):
    while chains:
        chains = advance(chains)


def edge_pass(members, edges, refs, write, chain_of):
    base, pre, table, gather, w2, gain, split = refs
    cuts = [slice(r, r + CHUNK) for r in range(0, edges, CHUNK)]
    middle = edges - CHUNK // 2
    items = [(m, rows) for m in range(members) for rows in cuts]
    items[-1:] = [(members - 1, slice(edges - CHUNK, middle)), (members - 1, slice(middle, edges))]

    def hidden_of(m, rows):
        return jnp.concatenate(
            [silu_of_half(pre[h, m, rows, :] + dot(gather[rows, split:], table[h, m, split:, :])) for h in range(2)], -1
        )

    ahead = hidden_of(*items[0])
    chains = []
    for i, (m, rows) in enumerate(items):
        hidden = ahead
        if i + 1 < len(items):
            ahead = hidden_of(*items[i + 1])
        update = scaled(wide_dot(hidden, w2), gain)
        write(m, rows, (base[m, rows, :] + update).astype(BF16))
        chains = advance(chains)
        if rows.stop == edges:
            chains.append(chain_of(m))
    drain(chains)


def exchange_body(
    sizes,
    node_in, edge_in, senders_in, receivers_in, counts_in, halo_in, long_in,
    ef_in, es_in, nf_in, ns_in, eg_in, eb_in, ng_in, nb_in,
    node_base, edge_base, pre, node_pre, table, gather, scatter, weights, norms,
    node, edge, first, ids_v, count_s, halo_v, long_v, picked, picker, sent_scatter, sent, sent_base, sent_pre,
    outgoing, incoming,
    wr_sem, in_sem,
    node_sem, halo_sem, long_sem, ids_sem, count_sem, edge_sem, norm_sem, own_sem, ws_sem, out_sem,
):
    n, layers, members, nodes, edges, width, side_rows, slots = sizes
    me = lax.axis_index("dom")
    core = lax.axis_index("mem")
    halves = 2
    other = 1 - core
    split = 2 * nodes
    near_rows = 2 * side_rows + n * slots
    everyone = range(members)

    pltpu.make_async_copy(halo_in, halo_v, halo_sem).start()
    pltpu.make_async_copy(long_in.at[me], long_v, long_sem).start()
    pltpu.make_async_copy(node_in, node, node_sem).start()

    barrier = pltpu.get_barrier_semaphore()
    pl.semaphore_signal(barrier, inc=1, device_id={"mem": other})
    for step in range(1, n):
        pl.semaphore_signal(barrier, inc=1, device_id={"dom": lax.rem(me + step, n)})

    def whole(ref, sem):
        return pltpu.make_async_copy(ref, ref, sem)

    blocks = ((ef_in, 0, 3), (es_in, 0, 1), (nf_in, 1, 2), (ns_in, 3, 1))

    def place(l, k, part):
        src, start, count = blocks[k]
        held = weights if k else first
        return src.at[l], held.at[l, part, start * width : (start + count) * width]

    pltpu.make_async_copy(senders_in, ids_v.at[0], ids_sem).start()
    pltpu.make_async_copy(receivers_in, ids_v.at[1], ids_sem).start()
    pltpu.make_async_copy(counts_in, count_s, count_sem).start()
    pltpu.make_async_copy(*place(0, 0, core), own_sem.at[0, 0]).start()
    pltpu.make_async_copy(edge_in, edge, edge_sem).start()
    for k, src in enumerate((eg_in, eb_in, ng_in, nb_in)):
        pltpu.make_async_copy(src, norms.at[k], norm_sem).start()
    for l in range(layers):
        for k in range(4):
            if (l, k) != (0, 0):
                pltpu.make_async_copy(*place(l, k, core), own_sem.at[l, min(k, 1)]).start()

    def wait_weights(l, group):
        whole((weights if group else first).at[l, core], own_sem.at[l, group]).wait()

    def wait_partner(l, group):
        whole((weights if group else first).at[l, other], wr_sem.at[l, group]).wait()

    def column(row):
        wide = round_up(row.shape[1], LANES)
        if wide > row.shape[1]:
            row = jnp.concatenate([row, jnp.zeros((1, wide - row.shape[1]), jnp.int32)], 1)
        return jnp.transpose(jnp.broadcast_to(row, (LANES, wide)))

    def one_hot(hits):
        return hits.astype(F32).astype(BF16)

    whole(halo_v, halo_sem).wait()
    whole(long_v, long_sem).wait()
    picked[: 2 * side_rows, :] = column(halo_v[...].reshape(1, 2 * side_rows))[: 2 * side_rows]
    for s in range(slots):
        picked[pl.ds(2 * side_rows + s, n, stride=slots), :] = column(long_v[s : s + 1, :])[:n]
    for c in range(nodes // LANES):
        lane = lax.broadcasted_iota(jnp.int32, picked.shape, 1) + c * LANES
        picker[:, c * LANES : (c + 1) * LANES] = one_hot(picked[...] == lane)

    span = side_rows // slots

    def stage(l, m, packed):
        outgoing[l, :, m] = packed.reshape(2 * span + n, slots, width)

    def partner_of(mask):
        target, bit = 0, 1
        while bit < n:
            target = target + lax.rem(me // bit + (mask // bit) % 2, 2) * bit
            bit *= 2
        return target

    if n & (n - 1):
        targets = [lax.rem(me + step, n) for step in range(1, n)]
    else:
        targets = [partner_of(mask) for mask in range(n - 1, 0, -1)]

    def send(l):
        pieces = [(side * span, (1 - side) * span, span, lax.rem(me + step, n)) for side, step in ((0, n - 1), (1, 1))]
        pieces += [(2 * span + target, 2 * span + me, 1, target) for target in targets]
        pieces = pieces[2:3] + pieces[:2] + pieces[3:]
        for start, landing, count, target in pieces:
            pltpu.make_async_remote_copy(
                src_ref=outgoing.at[l, pl.ds(start, count)],
                dst_ref=incoming.at[l, pl.ds(landing, count)],
                send_sem=out_sem.at[l],
                recv_sem=in_sem.at[l],
                device_id={"dom": target},
            ).start()
        mine = pl.ds(2 * span + me, 1)
        pltpu.make_async_copy(outgoing.at[l, mine], incoming.at[l, mine], in_sem.at[l]).start()

    whole(node, node_sem).wait()
    for m in everyone:
        rows = dot(picker[...], node[m]).astype(BF16)
        sent[m] = rows
        stage(0, m, rows)
    pl.semaphore_wait(barrier, n)
    send(0)
    for l in range(layers):
        for k in range(4):
            src, dst = place(l, k, core)
            pltpu.make_async_remote_copy(
                src_ref=src,
                dst_ref=dst,
                send_sem=ws_sem.at[min(k, 1)],
                recv_sem=wr_sem.at[l, min(k, 1)],
                device_id={"mem": other},
            ).start()

    whole(ids_v, ids_sem).wait()
    pltpu.make_async_copy(counts_in, count_s, count_sem).wait()
    count = count_s[0]
    depth = gather.shape[1]
    senders = column(ids_v[0:1, :])
    receiver_row = ids_v[1:2, :]
    receivers = column(receiver_row) + nodes
    senders = jnp.where(senders < nodes, senders, senders + nodes)
    for c in range(depth // LANES):
        lane = lax.broadcasted_iota(jnp.int32, (edges, LANES), 1) + c * LANES
        hits = ((senders == lane) | (receivers == lane)) & live_rows(0, edges, count)
        gather[:, c * LANES : (c + 1) * LANES] = one_hot(hits)
    row = lax.broadcasted_iota(jnp.int32, (nodes, edges), 0)
    scatter[...] = one_hot(jnp.broadcast_to(receiver_row, (nodes, edges)) == row)
    sent_scatter[...] = dot(picker[...], scatter[...]).astype(BF16)
    far_base = split + near_rows
    if far_base < depth:
        for h in range(halves):
            for m in everyone:
                table[h, m, far_base:, :] = jnp.zeros((depth - far_base, table.shape[3]), BF16)
    whole(edge, edge_sem).wait()
    whole(norms, norm_sem).wait()

    def prepare(l, h):
        w1 = first.at[l, h]
        for m in everyone:
            table[h, m, :nodes, :] = (0.5 * dot(node[m], w1[width : 2 * width, :])).astype(BF16)
            table[h, m, nodes:split, :] = (0.5 * dot(node[m], w1[2 * width : 3 * width, :])).astype(BF16)
        for m in everyone:
            pre[h, m] = 0.5 * dot(edge[m], w1[:width, :]) + dot(gather[:, :split], table[h, m, :split, :])

    def centre(l, start):
        for r in range(start, start + width, LANES):
            rows = slice(r, r + LANES)
            values = [weights[l, h, rows, :].astype(F32) for h in range(halves)]
            average = sum(jnp.sum(v, -1, keepdims=True) for v in values) / width
            for h in range(halves):
                weights[l, h, rows, :] = (values[h] - average).astype(BF16)

    def edge_prepare(l):
        for m in everyone:
            for r in range(0, edges, LANES):
                rows = slice(r, r + LANES)
                live = live_rows(r, LANES, count)
                kept = edge[m, rows, :].astype(F32)
                edge_base[m, rows, :] = jnp.where(live, kept + norms[1, l : l + 1, :], 0.0)
                if l == 0:
                    edge[m, rows, :] = jnp.where(live, kept, 0.0).astype(BF16)

    def node_prepare(l):
        centre(l, 0)
        centre(l, 3 * width)
        for m in everyone:
            node_base[m] = node[m].astype(F32) + norms[3, l : l + 1, :]
            if l < layers - 1:
                sent_base[m * near_rows : (m + 1) * near_rows, :] = sent[m].astype(F32) + norms[3, l : l + 1, :]
        for h in range(halves):
            w3a = weights[l, h, width : 2 * width, :]
            for m in everyone:
                if l < layers - 1:
                    sent_pre[m, h] = 0.5 * dot(sent[m], w3a)
                node_pre[m, h] = 0.5 * dot(node[m], w3a)

    def receive(l, ms):
        whole(incoming.at[l], in_sem.at[l]).wait()
        for m in ms:
            near = incoming[l, :, m].reshape(near_rows, width)
            for h in range(halves):
                table[h, m, split : split + near_rows, :] = (
                    0.5 * dot(near, first[l, h, width : 2 * width, :])
                ).astype(BF16)

    edge_prepare(0)
    wait_weights(0, 0)
    prepare(0, core)
    wait_partner(0, 0)
    prepare(0, other)
    wait_weights(0, 1)
    wait_partner(0, 1)
    node_prepare(0)

    for l in range(layers):
        w = weights.at[l]
        receive(l, everyone)
        if l == layers - 1:
            continue
        node_refs = (
            w.at[:, 2 * width : 3 * width], w.at[:, 3 * width :],
            norms[2, l : l + 1, :],
        )
        edge_refs = (
            edge_base, pre, table, gather, w.at[:, :width],
            norms[0, l : l + 1, :], split,
        )

        def write(m, rows, value):
            edge[m, rows, :] = value

        def sent_chain(m):
            rows = slice(m * near_rows, (m + 1) * near_rows)

            def finish(fresh):
                if l + 1 < layers - 1:
                    sent[m] = fresh
                stage(l + 1, m, fresh)

            return node_chain(
                lambda: dot(sent_scatter[...], edge[m]).astype(BF16),
                lambda: sent_base[rows, :], lambda h: sent_pre[m, h], node_refs, finish,
            )

        def kept_chain(m):
            def finish(fresh):
                node[m] = fresh

            return node_chain(
                lambda: dot(scatter[...], edge[m]).astype(BF16),
                lambda: node_base[m], lambda h: node_pre[m, h], node_refs, finish,
            )

        edge_pass(members, edges, edge_refs, write, sent_chain)
        send(l + 1)
        drain([kept_chain(m) for m in everyone])
        edge_prepare(l + 1)
        wait_weights(l + 1, 0)
        wait_partner(l + 1, 0)
        for h in range(halves):
            prepare(l + 1, h)
        wait_weights(l + 1, 1)
        wait_partner(l + 1, 1)
        node_prepare(l + 1)

    whole(first.at[:, core], ws_sem.at[0]).wait()
    whole(weights.at[:, core], ws_sem.at[1]).wait()
    for l in range(layers):
        whole(outgoing.at[l, : 2 * span + n - 1], out_sem.at[l]).wait()


def exchange_kernel(sizes, *refs):
    layers, dma = sizes[1], pltpu.SemaphoreType.DMA
    local = [dma(())] * 7 + [dma((layers, 2)), dma((2,)), dma((layers,))]
    pl.run_scoped(functools.partial(exchange_body, sizes, *refs), *local)


def finish_body(
    sizes,
    node_base, edge_base, pre, node_pre, table, gather, scatter, weights, norms,
    node_out, edge_out, edge_new, node_new, edge_sem, node_sem,
):
    n, layers, members, nodes, edges, width, side_rows, slots = sizes
    l = layers - 1
    w = weights.at[l]
    edge_refs = (
        edge_base, pre, table, gather, w.at[:, :width],
        norms[0, l : l + 1, :], 2 * nodes,
    )
    node_refs = (
        w.at[:, 2 * width : 3 * width], w.at[:, 3 * width :],
        norms[2, l : l + 1, :],
    )

    def write(m, rows, value):
        edge_new[m, rows, :] = value
        pltpu.make_async_copy(edge_new.at[m, rows], edge_out.at[m, rows], edge_sem).start()

    def chain_of(m):
        def finish(fresh):
            node_new[m] = fresh
            pltpu.make_async_copy(node_new.at[m], node_out.at[m], node_sem).start()

        return node_chain(
            lambda: dot(scatter[...], edge_new[m]).astype(BF16),
            lambda: node_base[m], lambda h: node_pre[m, h], node_refs, finish,
        )

    edge_pass(members, edges, edge_refs, write, chain_of)
    pltpu.make_async_copy(edge_new, edge_out, edge_sem).wait()
    pltpu.make_async_copy(node_new, node_out, node_sem).wait()


def finish_kernel(sizes, *refs):
    dma = pltpu.SemaphoreType.DMA
    pl.run_scoped(functools.partial(finish_body, sizes, *refs), dma(()), dma(()))


def solution(mesh):
    n = mesh.shape["dom"]

    def step(
        node, edge, senders, receivers, counts, halo_send, long_send, ef, es, nf, ns, eg, eb, ng, nb
    ):
        members, nodes, width = node.shape
        edges = edge.shape[1]
        layers = ef.shape[0]
        side_rows = halo_send.shape[0] // 2
        slots = long_send.shape[-1]
        long_rows = jnp.swapaxes(long_send, 1, 2)
        near_rows = 2 * side_rows + n * slots
        depth = 2 * nodes + round_up(near_rows, LANES)
        sizes = (n, layers, members, nodes, edges, width, side_rows, slots)
        half = width // 2
        hbm = pl.BlockSpec(memory_space=pltpu.HBM)
        vmem = pl.BlockSpec(memory_space=pltpu.VMEM)
        dma = pltpu.SemaphoreType.DMA
        kept = [
            (node.shape, F32),
            (edge.shape, F32),
            ((2, members, edges, half), F32),
            ((members, 2, nodes, half), F32),
            ((2, members, depth, half), BF16),
            ((edges, depth), BF16),
            ((nodes, edges), BF16),
            ((layers, 2, 4 * width, half), BF16),
            ((4,) + eg.shape, F32),
        ]
        state = pl.pallas_call(
            functools.partial(exchange_kernel, sizes),
            out_shape=tuple(pltpu.VMEM(shape, kind) for shape, kind in kept),
            in_specs=[hbm] * 15,
            out_specs=(vmem,) * len(kept),
            scratch_shapes=[
                pltpu.VMEM(node.shape, BF16),
                pltpu.VMEM(edge.shape, BF16),
                pltpu.VMEM((layers, 2, ef.shape[1], half), BF16),
                pltpu.VMEM((2,) + senders.shape, jnp.int32),
                pltpu.SMEM(counts.shape, jnp.int32),
                pltpu.VMEM(halo_send.shape, jnp.int32),
                pltpu.VMEM(long_rows.shape[1:], jnp.int32),
                pltpu.VMEM((near_rows, LANES), jnp.int32),
                pltpu.VMEM((near_rows, nodes), BF16),
                pltpu.VMEM((near_rows, edges), BF16),
                pltpu.VMEM((members, near_rows, width), BF16),
                pltpu.VMEM((members * near_rows, width), F32),
                pltpu.VMEM((members, 2, near_rows, half), F32),
                pltpu.VMEM((layers, near_rows // slots, members, slots, width), BF16),
                pltpu.VMEM((layers, near_rows // slots, members, slots, width), BF16),
                dma((layers, 2)),
                dma((layers,)),
            ],
            compiler_params=pltpu.CompilerParams(
                collective_id=0, has_side_effects=True, vmem_limit_bytes=51 * 1024 * 1024
            ),
        )(node, edge, senders, receivers, counts, halo_send, long_rows, ef, es, nf, ns, eg, eb, ng, nb)
        return pl.pallas_call(
            functools.partial(finish_kernel, sizes),
            out_shape=(
                jax.ShapeDtypeStruct(node.shape, BF16),
                jax.ShapeDtypeStruct(edge.shape, BF16),
            ),
            in_specs=[vmem] * len(kept),
            out_specs=(hbm, hbm),
            scratch_shapes=[
                pltpu.VMEM(edge.shape, BF16),
                pltpu.VMEM(node.shape, BF16),
            ],
            compiler_params=pltpu.CompilerParams(vmem_limit_bytes=40 * 1024 * 1024),
        )(*state)

    shared, halved = P(), P(None, None, "mem")
    parts = P("mem", "dom", None)
    placed = (parts,) * 2 + (P("dom"),) * 4 + (shared,) + (halved,) * 4 + (shared,) * 4
    return jax.shard_map(step, mesh=mesh, in_specs=placed, out_specs=(parts, parts), check_vma=False)
```
